64 devices in a mesh: rep: 4 (over x, y), dp: 16 (over z, core).
Axes of the slice: x: 2, y: 2, z: 8, core: 2. Of those that a mesh axis runs over, the one named last changes fastest.
The devices are a block of a 4x4x8 slice.
Arguments:
- x: bfloat16 [64, 1024, 896], P(('rep', 'dp')), parts along dimension 0
- dy: bfloat16 [64, 1024, 896], P(('rep', 'dp')), parts along dimension 0
- w_gate: bfloat16 [2, 896, 2560], replicated
- w_up: bfloat16 [2, 896, 2560], replicated
- w_down: bfloat16 [2, 2560, 896], replicated
- m_w_gate: float32 [2, 896, 2560], P(None, 'dp')
- m_w_up: float32 [2, 896, 2560], P(None, 'dp')
- m_w_down: float32 [2, 2560, 896], P(None, 'dp')
- v_w_gate: float32 [2, 896, 2560], P(None, 'dp')
- v_w_up: float32 [2, 896, 2560], P(None, 'dp')
- v_w_down: float32 [2, 2560, 896], P(None, 'dp')
Outputs:
- output 1: bfloat16 [8, 896, 2560], P('rep'), parts along dimension 0
- output 2: bfloat16 [8, 896, 2560], P('rep'), parts along dimension 0
- output 3: bfloat16 [8, 2560, 896], P('rep'), parts along dimension 0
- output 4: float32 [8, 896, 2560], P('rep', 'dp'), parts along dimension 0
- output 5: float32 [8, 896, 2560], P('rep', 'dp'), parts along dimension 0
- output 6: float32 [8, 2560, 896], P('rep', 'dp'), parts along dimension 0
- output 7: float32 [8, 896, 2560], P('rep', 'dp'), parts along dimension 0
- output 8: float32 [8, 896, 2560], P('rep', 'dp'), parts along dimension 0
- output 9: float32 [8, 2560, 896], P('rep', 'dp'), parts along dimension 0
There are 4 independent parts. The reference program is written for one: setup_inputs(seed, part) draws one part's arguments, and reference() takes and returns one part's arrays. A program takes and returns all parts, laid end to end along the dimension named above; an argument that names none is the same for every part.
All inputs are finite; a program needn't handle non-finite values.
Results may differ from the reference program's by a relative error of at most 0.022.
Values are sent between devices in bfloat16 or wider.
A program may use at most 768 MiB of HBM per device.

```python
import jax
import jax.numpy as jnp
from jax import lax

SEQUENCES = 16
TOKENS = 1024
D = 896
FF = 2560
LAYERS = 2
NAMES = ("w_gate", "w_up", "w_down")
SHAPES = {"w_gate": (LAYERS, D, FF), "w_up": (LAYERS, D, FF), "w_down": (LAYERS, FF, D)}


def bump(key, n, height):
    away = (jnp.arange(n, dtype=jnp.int32) - jax.random.randint(key, (), 0, n, jnp.int32)) % n
    return jnp.where(away < n // 8, height, 1.0)


def together(key, own, strength):
    shared = jax.random.normal(key, own.shape[1:], jnp.float32)
    return (own + strength * shared) * lax.rsqrt(1 + strength * strength)


def setup_inputs(seed: int = 0, part: int = 0) -> dict:
    kx, kdy, ka, kb, kz, kf, kh, kl, *keys = jax.random.split(jax.random.key(seed), 8 + 3 * len(NAMES))
    kx, kdy, ka, kb = (jax.random.fold_in(k, part) for k in (kx, kdy, ka, kb))
    kw, km, kv = (keys[i::3] for i in range(3))
    shape = (SEQUENCES, TOKENS, D)
    much_x, much_dy = jax.random.uniform(kz, (2,), jnp.float32, 0.0, 1.0)
    loud = 2.0 ** jax.random.uniform(jax.random.fold_in(kz, 1), (), jnp.float32, -1.0, 2.0)
    layers = 2.0 ** jax.random.uniform(kl, (LAYERS, 1, 1), jnp.float32, -1.0, 1.0)
    x = together(ka, jax.random.normal(kx, shape, jnp.float32), much_x) * bump(kf, D, 4.0)
    dy = together(kb, jax.random.normal(kdy, shape, jnp.float32), much_dy)
    drawn = {"x": x.astype(jnp.bfloat16), "dy": (loud * dy * (SEQUENCES * TOKENS) ** -0.5).astype(jnp.bfloat16)}
    for key, name in zip(kw, NAMES, strict=True):
        w = jax.random.normal(key, SHAPES[name], jnp.float32) * SHAPES[name][1] ** -0.5
        drawn[name] = (w * {"w_gate": 1.0, "w_up": bump(kh, FF, 4.0), "w_down": layers}[name]).astype(jnp.bfloat16)
    for key, name in zip(km, NAMES, strict=True):
        drawn[f"m_{name}"] = 0.1 * jax.random.normal(key, SHAPES[name], jnp.float32)
    for key, name in zip(kv, NAMES, strict=True):
        drawn[f"v_{name}"] = jax.random.uniform(key, SHAPES[name], jnp.float32, 0.005, 0.015)
    return drawn


def matmul(a, w):
    return jnp.dot(a, w, preferred_element_type=jnp.float32).astype(jnp.bfloat16)


def normed(h):
    wide = h.astype(jnp.float32)
    scale = lax.rsqrt(jnp.mean(wide**2, -1, keepdims=True) + 1e-6)
    return (wide * scale).astype(jnp.bfloat16)


def layer(h, w):
    a = normed(h)
    gate = jnp.dot(a, w["w_gate"], preferred_element_type=jnp.float32)
    up = jnp.dot(a, w["w_up"], preferred_element_type=jnp.float32)
    return h + matmul((jax.nn.silu(gate) * up).astype(jnp.bfloat16), w["w_down"])


def adamw(w, m, v, g):
    m = 0.9 * m + 0.1 * g
    v = 0.95 * v + 0.05 * g * g
    step = m * lax.rsqrt(v + 1e-8) + 0.1 * w
    return (w - 0.02 * step).astype(jnp.bfloat16), m, v


def clipped(gradients, sum_of_squares, count):
    factor = jnp.minimum(1.0, 0.5 * lax.rsqrt(sum_of_squares / count + 1e-30))
    return [g * factor for g in gradients]


def stack(weights, h):
    return lax.scan(lambda h, w: (layer(h, w), None), h, weights)[0]


def reference(x, dy, w_gate, w_up, w_down, m_w_gate, m_w_up, m_w_down, v_w_gate, v_w_up, v_w_down):
    weights = dict(zip(NAMES, (w_gate, w_up, w_down), strict=True))

    def take(so_far, sequence):
        h, by_y = sequence
        _, back = jax.vjp(lambda w: stack(w, h), weights)
        return jax.tree.map(lambda total, term: total + term.astype(jnp.float32), so_far, back(by_y)[0]), None

    none_yet = {name: jnp.zeros(w.shape, jnp.float32) for name, w in weights.items()}
    by_weights, _ = lax.scan(take, none_yet, (x, dy))
    gradients = [by_weights[name].astype(jnp.bfloat16).astype(jnp.float32) for name in NAMES]
    gradients = clipped(gradients, sum(jnp.sum(g * g) for g in gradients), sum(g.size for g in gradients))
    new = [
        adamw(w.astype(jnp.float32), m, v, g)
        for w, m, v, g in zip((w_gate, w_up, w_down), (m_w_gate, m_w_up, m_w_down), (v_w_gate, v_w_up, v_w_down), gradients, strict=True)
    ]
    return tuple(one[which] for which in range(3) for one in new)
```

```python
import jax
import jax.numpy as jnp
from jax import lax
from jax.sharding import PartitionSpec as P

NAMES = ("w_gate", "w_up", "w_down")


def matmul(a, w):
    return jnp.dot(a, w, preferred_element_type=jnp.float32).astype(jnp.bfloat16)


def normed(h):
    wide = h.astype(jnp.float32)
    scale = lax.rsqrt(jnp.mean(wide**2, -1, keepdims=True) + 1e-6)
    return (wide * scale).astype(jnp.bfloat16)


def layer(h, w):
    a = normed(h)
    gate = jnp.dot(a, w["w_gate"], preferred_element_type=jnp.float32)
    up = jnp.dot(a, w["w_up"], preferred_element_type=jnp.float32)
    return h + matmul((jax.nn.silu(gate) * up).astype(jnp.bfloat16), w["w_down"])


def adamw(w, m, v, g):
    m = 0.9 * m + 0.1 * g
    v = 0.95 * v + 0.05 * g * g
    step = m * lax.rsqrt(v + 1e-8) + 0.1 * w
    return (w - 0.02 * step).astype(jnp.bfloat16), m, v


def stack(weights, h):
    for w in weights:
        h = layer(h, w)
    return h


def solution(mesh):
    def of_a_device(x, dy, *arrays):
        stacked, m, v = (arrays[i : i + 3] for i in (0, 3, 6))
        layers = stacked[0].shape[0]
        place = lax.axis_index("dp")
        weights = [{n: w[i] for n, w in zip(NAMES, stacked)} for i in range(layers)]
        _, back = jax.vjp(lambda w: stack(w, x[0]), weights)
        (terms,) = back(dy[0])
        sums = [
            {n: lax.psum_scatter(terms[i][n], "dp", scatter_dimension=0, tiled=True).astype(jnp.float32) for n in NAMES}
            for i in range(layers)
        ]
        square = lax.psum(sum(jnp.sum(g * g) for one in sums for g in one.values()), "dp")
        count = sum(w.size for w in stacked)
        factor = jnp.minimum(1.0, 0.5 * lax.rsqrt(square / count + 1e-30))
        new = []
        for n, w, m1, v1 in zip(NAMES, stacked, m, v):
            g = jnp.stack([one[n] for one in sums]) * factor
            rows = m1.shape[1]
            mine = lax.dynamic_slice_in_dim(w, place * rows, rows, 1)
            w1, m1, v1 = adamw(mine.astype(jnp.float32), m1, v1, g)
            new.append((lax.all_gather(w1, "dp", axis=1, tiled=True), m1, v1))
        return tuple(one[which] for which in range(3) for one in new)

    seq, whole, rows = P(("rep", "dp")), P(), P(None, "dp")
    return jax.shard_map(
        of_a_device,
        mesh=mesh,
        in_specs=(seq, seq) + (whole,) * 3 + (rows,) * 6,
        out_specs=(P("rep"),) * 3 + (P("rep", "dp"),) * 6,
        check_vma=False,
    )
```

```python
import functools

import jax
import jax.numpy as jnp
from jax import lax
from jax.experimental import pallas as pl
from jax.experimental.pallas import tpu as pltpu
from jax.sharding import PartitionSpec as P

MESH = pl.DeviceIdType.MESH
BF, F32 = jnp.bfloat16, jnp.float32
LANES = 128
TILE = 512
QUARTERS = TILE // LANES
ROWS = 512
LAG = 2
LAG_PARTNER = 1
RING_GRAD, RING_SUM, RING_PARTNER = 16, 10, 4
VMEM_LIMIT = 66_000_000


def nn(a, b):
    return lax.dot_general(a, b, (((1,), (0,)), ((), ())), preferred_element_type=F32)


def nt(a, b):
    return lax.dot_general(a, b, (((1,), (1,)), ((), ())), preferred_element_type=F32)


def tn(a, b):
    return lax.dot_general(a, b, (((0,), (0,)), ((), ())), preferred_element_type=F32)


def normed(h):
    wide = h.astype(F32)
    scale = lax.rsqrt(jnp.mean(wide * wide, -1, keepdims=True) + 1e-6)
    return (wide * scale).astype(BF)


def sigmoid(x):
    return 1.0 / (1.0 + jnp.exp(-x))


def forward_kernel(tiles, x_ref, wg_ref, wu_ref, wd_ref, a_ref, at_ref, h_ref, b_ref, bt_ref, acc):
    t = pl.program_id(0)

    @pl.when(t == 0)
    def _():
        a = normed(x_ref[...])
        a_ref[...] = a
        at_ref[...] = a.T
        acc[...] = jnp.zeros_like(acc)

    for r in range(0, x_ref.shape[0], ROWS):
        a = a_ref[r : r + ROWS, :]
        gate = nn(a, wg_ref[...])
        up = nn(a, wu_ref[...])
        act = (gate * sigmoid(gate) * up).astype(BF)
        acc[r : r + ROWS, :] += nn(act, wd_ref[...])

    @pl.when(t == tiles - 1)
    def _():
        h = (x_ref[...].astype(F32) + acc[...].astype(BF).astype(F32)).astype(BF)
        h_ref[...] = h
        b = normed(h)
        b_ref[...] = b
        bt_ref[...] = b.T


def forward(x, wg, wu, wd, layer):
    tokens, d = x.shape
    tiles = wg.shape[2] // TILE
    one = lambda s: pl.BlockSpec(s, lambda t: (0, 0))
    return pl.pallas_call(
        functools.partial(forward_kernel, tiles),
        grid=(tiles,),
        in_specs=[
            one((tokens, d)),
            pl.BlockSpec((None, d, TILE), lambda t: (layer, 0, t)),
            pl.BlockSpec((None, d, TILE), lambda t: (layer, 0, t)),
            pl.BlockSpec((None, TILE, d), lambda t: (layer, t, 0)),
        ],
        out_specs=[one((tokens, d)), one((d, tokens)), one((tokens, d)), one((tokens, d)), one((d, tokens))],
        out_shape=[jax.ShapeDtypeStruct(s, BF) for s in ((tokens, d), (d, tokens), (tokens, d), (tokens, d), (d, tokens))],
        scratch_shapes=[pltpu.VMEM((tokens, d), F32)],
        compiler_params=pltpu.CompilerParams(vmem_limit_bytes=60_000_000),
        name="forward",
    )(x, wg, wu, wd)


def places(n):
    me = lax.axis_index("dp")
    chips = n // 2
    z, c = me // 2, lax.rem(me, 2)
    plus = lax.rem(z + 1, chips) * 2 + c
    minus = lax.rem(z + chips - 1, chips) * 2 + c
    return me, z, c, z * 2 + 1 - c, plus, minus


def enter(others):
    barrier = pltpu.get_barrier_semaphore()
    for o in others:
        pl.semaphore_signal(barrier, inc=1, device_id={"dp": o}, device_id_type=MESH)
    pl.semaphore_wait(barrier, len(others))


def backward_kernel(
    n, layers, tiles, rows,
    a0_h, at0_h, a1_h, at1_h, h1_h, dy_h, wg_h, wu_h, wd_h,
    out, squares,
    a, at, h, dy, wg, wu, wd, act, dgate, dup, acc,
    grad, partner_sum, total, hop_in,
    d_send, d_recv, r_send, r_recv, load_sem, w_sem,
):
    chips, half = n // 2, n // 4
    per_layer = tiles * QUARTERS + tiles * 2
    chunks = layers * per_layer
    slots = 2 * LAG
    me, z, c, partner, plus, minus = places(n)
    tokens, d = a.shape

    def load(src, dst, i):
        return pltpu.make_async_copy(src, dst, load_sem.at[i])

    def weights(layer, t, only=None):
        b = lax.rem(t, 2)
        at_cols = pl.ds(pl.multiple_of(t * TILE, TILE), TILE)
        return [
            pltpu.make_async_copy(wg_h.at[layer, :, at_cols], wg.at[b], w_sem.at[0, b]),
            pltpu.make_async_copy(wu_h.at[layer, :, at_cols], wu.at[b], w_sem.at[1, b]),
            pltpu.make_async_copy(wd_h.at[layer, at_cols, :], wd.at[b], w_sem.at[2, b]),
        ]

    first = [load(a1_h, a, 0), load(dy_h, dy, 1), load(at1_h, at, 2), load(h1_h, h, 3)]
    for one in first:
        one.start()
    for one in weights(layers - 1, jnp.int32(0)):
        one.start()
    squares[...] = jnp.zeros_like(squares)
    enter([partner, plus, minus])

    def to_partner(k):
        b = lax.rem(k, RING_PARTNER)
        return pltpu.make_async_remote_copy(
            src_ref=grad.at[lax.rem(k, RING_GRAD), 1 - c],
            dst_ref=partner_sum.at[b],
            send_sem=d_send.at[b],
            recv_sem=d_recv.at[b],
            device_id={"dp": partner},
            device_id_type=MESH,
        )

    def hop(way, s, slot):
        k = lax.rem(slot - LAG_PARTNER - LAG * s, RING_SUM)
        b = lax.rem(slot, slots)
        far = lax.rem(z + (half - s if way == 0 else chips - half + s), chips)
        src, dst = total.at[k, far], hop_in.at[way, s, b]
        if s == 0:
            src, dst = src.at[way], dst.at[way]
        return pltpu.make_async_remote_copy(
            src_ref=src,
            dst_ref=dst,
            send_sem=r_send.at[way, s, b],
            recv_sem=r_recv.at[way, s, b],
            device_id={"dp": plus if way == 0 else minus},
            device_id_type=MESH,
        )

    def during(k):
        return (k >= 0) & (k < chunks)

    def slot(now):
        @pl.when(during(now))
        def _():
            to_partner(now).start()

        k0 = now - LAG_PARTNER

        @pl.when(during(k0))
        def _():
            to_partner(k0).wait()
            i, g, b = lax.rem(k0, RING_SUM), lax.rem(k0, RING_GRAD), lax.rem(k0, RING_PARTNER)
            for j in range(chips):
                total[i, j] = (grad[g, c, j].astype(F32) + partner_sum[b, j].astype(F32)).astype(BF)

        for s in range(1, half):
            k = now - LAG_PARTNER - LAG * s

            @pl.when(during(k))
            def _(k=k, s=s):
                i, b = lax.rem(k, RING_SUM), lax.rem(now - LAG, slots)
                for way in (0, 1):
                    hop(way, s - 1, now - LAG).wait()
                    far = lax.rem(z + (half - s if way == 0 else chips - half + s), chips)
                    if s == 1:
                        total[i, far, way] = (total[i, far, way].astype(F32) + hop_in[way, 0, b, way].astype(F32)).astype(BF)
                    else:
                        total[i, far] = (total[i, far].astype(F32) + hop_in[way, s - 1, b].astype(F32)).astype(BF)

        k1 = now - LAG_PARTNER - LAG * half

        @pl.when(during(k1))
        def _():
            b = lax.rem(now - LAG, slots)
            for way in (0, 1):
                hop(way, half - 1, now - LAG).wait()
            own = total[lax.rem(k1, RING_SUM), z].astype(F32)
            g = (own + hop_in[0, half - 1, b].astype(F32) + hop_in[1, half - 1, b].astype(F32)).astype(BF)
            out[k1] = g
            wide = g.astype(F32)
            squares[...] += wide[0] * wide[0] + wide[1] * wide[1]

        for s in range(half):
            k = now - LAG_PARTNER - LAG * s

            @pl.when(during(k))
            def _(s=s):
                for way in (0, 1):
                    hop(way, s, now).start()

    def elementwise(b, t, r):
        at_rows = pl.ds(r, ROWS)
        gate = nn(a[at_rows, :], wg[b])
        up = nn(a[at_rows, :], wu[b])
        by_act = nt(dy[at_rows, :], wd[b]).astype(BF).astype(F32)
        s = sigmoid(gate)
        silu = gate * s
        act[t, at_rows, :] = (silu * up).astype(BF)
        dup[t, at_rows, :] = (by_act * silu).astype(BF)
        dgate[t, at_rows, :] = (by_act * up * (s * (1.0 + gate * (1.0 - s)))).astype(BF)

    def wide_grad(source, first_chunk, t):
        for p in range(2):
            g = nn(at[p * (d // 2) : (p + 1) * (d // 2), :], source[t])
            for i in range(n // 2):
                dev = p * (n // 2) + i
                for q in range(QUARTERS):
                    k = lax.rem(first_chunk + q // 2, RING_GRAD)
                    grad[k, dev % 2, dev // 2, q % 2] = g[i * rows : (i + 1) * rows, q * LANES : (q + 1) * LANES].astype(BF)

    def tall_grad(t, base):
        acc[:TILE, :] = tn(act[t], dy[...])

        def group(i, _):
            g = t * (TILE // 8) + i
            per_dev = tiles * TILE // n // 8
            dev, rest = g // per_dev, lax.rem(g, per_dev)
            k = lax.rem(base + tiles * QUARTERS + rest // 2, RING_GRAD)
            eight = acc[pl.ds(pl.multiple_of(i * 8, 8), 8), :]
            stacked = jnp.concatenate([eight[:, q * LANES : (q + 1) * LANES] for q in range(d // LANES)], axis=0)
            grad[k, lax.rem(dev, 2), dev // 2, lax.rem(rest, 2)] = stacked.astype(BF)
            return 0

        lax.fori_loop(0, TILE // 8, group, 0, unroll=4)

    def to_states(layer, base):
        for which, (source, w, w_h) in enumerate(((dgate, wg, wg_h), (dup, wu, wu_h))):

            def copy(t, w=w, w_h=w_h, which=which):
                b = lax.rem(t, 2)
                cols = pl.ds(pl.multiple_of(t * TILE, TILE), TILE)
                return pltpu.make_async_copy(w_h.at[layer, :, cols], w.at[b], w_sem.at[which, b])

            copy(jnp.int32(0)).start()
            acc[...] = jnp.zeros_like(acc)

            def one(t, _, source=source, w=w, which=which, copy=copy):
                copy(t).wait()

                @pl.when(t + 1 < tiles)
                def _():
                    copy(t + 1).start()

                for r in range(0, tokens, ROWS):
                    acc[r : r + ROWS, :] += nt(source[t, r : r + ROWS, :], w[lax.rem(t, 2)])

                @pl.when(t < 4)
                def _():
                    slot(base + tiles * QUARTERS + which * 4 + t)

                return 0

            lax.fori_loop(0, tiles, one, 0)
            if which == 0:
                a[...] = acc[...].astype(BF)

        def norm(i, _):
            at_rows = pl.ds(pl.multiple_of(i * 64, 64), 64)
            by_a = (a[at_rows, :].astype(F32) + acc[at_rows, :].astype(BF).astype(F32)).astype(BF).astype(F32)
            wide = h[at_rows, :].astype(F32)
            scale = lax.rsqrt(jnp.mean(wide * wide, -1, keepdims=True) + 1e-6)
            along = jnp.mean(by_a * wide, -1, keepdims=True)
            by_h = (by_a * scale - wide * (scale * scale * scale * along)).astype(BF)
            dy[at_rows, :] = (dy[at_rows, :].astype(F32) + by_h.astype(F32)).astype(BF)
            return 0

        lax.fori_loop(0, tokens // 64, norm, 0)

    for one in first:
        one.wait()
    for step in range(layers):
        layer = layers - 1 - step
        base = step * per_layer

        def tile(t, _, layer=layer, base=base):
            b = lax.rem(t, 2)
            for one in weights(layer, t):
                one.wait()

            @pl.when(t + 1 < tiles)
            def _():
                for one in weights(layer, t + 1):
                    one.start()

            at_chunk = base + t * QUARTERS
            for i, r in enumerate(range(0, tokens, ROWS)):
                elementwise(b, t, r)
                slot(at_chunk - 2 + i)
            wide_grad(dgate, at_chunk, t)
            slot(at_chunk)
            wide_grad(dup, at_chunk + 2, t)
            slot(at_chunk + 1)
            return 0

        lax.fori_loop(0, tiles, tile, 0)
        if step < layers - 1:
            again = [load(at0_h, at, 2)]
            for one in again:
                one.start()

        def down(t, _, base=base):
            tall_grad(t, base)

            @pl.when(lax.rem(t, 2) == 1)
            def _():
                slot(base + tiles * QUARTERS - 2 + t // 2)

            return 0

        lax.fori_loop(0, tiles, down, 0)
        if step < layers - 1:
            to_states(layer, base)
            more = load(a0_h, a, 0)
            more.start()
            for one in weights(layer - 1, jnp.int32(0)):
                one.start()
            more.wait()
            for one in again:
                one.wait()

    def rest(i, _):
        slot(i)
        return 0

    lax.fori_loop((layers - 1) * per_layer + tiles * QUARTERS, chunks + LAG_PARTNER + LAG * half, rest, 0)


def backward(n, a0, at0, a1, at1, h1, dy, wg, wu, wd):
    layers, d, ff = wg.shape
    tokens = dy.shape[0]
    tiles, rows, chips, half = ff // TILE, d // n, n // 2, n // 4
    chunks = layers * (tiles * QUARTERS + tiles * 2)
    unit = (2, rows, LANES)
    hbm, vmem = pl.BlockSpec(memory_space=pl.ANY), pl.BlockSpec(memory_space=pltpu.VMEM)
    return pl.pallas_call(
        functools.partial(backward_kernel, n, layers, tiles, rows),
        in_specs=[hbm] * 9,
        out_specs=[vmem] * 2,
        out_shape=[jax.ShapeDtypeStruct((chunks,) + unit, BF), jax.ShapeDtypeStruct((rows, LANES), F32)],
        scratch_shapes=[
            pltpu.VMEM((tokens, d), BF),
            pltpu.VMEM((d, tokens), BF),
            pltpu.VMEM((tokens, d), BF),
            pltpu.VMEM((tokens, d), BF),
            pltpu.VMEM((2, d, TILE), BF),
            pltpu.VMEM((2, d, TILE), BF),
            pltpu.VMEM((2, TILE, d), BF),
            pltpu.VMEM((tiles, tokens, TILE), BF),
            pltpu.VMEM((tiles, tokens, TILE), BF),
            pltpu.VMEM((tiles, tokens, TILE), BF),
            pltpu.VMEM((tokens, d), F32),
            pltpu.VMEM((RING_GRAD, 2, chips) + unit, BF),
            pltpu.VMEM((RING_PARTNER, chips) + unit, BF),
            pltpu.VMEM((RING_SUM, chips) + unit, BF),
            pltpu.VMEM((2, half, 2 * LAG) + unit, BF),
            pltpu.SemaphoreType.DMA((RING_PARTNER,)),
            pltpu.SemaphoreType.DMA((RING_PARTNER,)),
            pltpu.SemaphoreType.DMA((2, half, 2 * LAG)),
            pltpu.SemaphoreType.DMA((2, half, 2 * LAG)),
            pltpu.SemaphoreType.DMA((4,)),
            pltpu.SemaphoreType.DMA((3, 2)),
        ],
        compiler_params=pltpu.CompilerParams(collective_id=0, has_side_effects=True, vmem_limit_bytes=VMEM_LIMIT),
        name="backward",
    )(a0, at0, a1, at1, h1, dy, wg, wu, wd)


def update_kernel(n, layers, tiles, count, *refs):
    grads, squares = refs[:2]
    w_h, m_h, v_h = refs[2:5], refs[5:8], refs[8:11]
    w_out, m_out, v_out = refs[11:14], refs[14:17], refs[17:20]
    w_in, m_in, v_in = refs[20:23], refs[23:26], refs[26:29]
    everyone, load_sem, store_sem, s_send, s_recv, r_send, r_recv, d_send, d_recv = refs[29:]
    chips, half = n // 2, n // 4
    me, z, c, partner, plus, minus = places(n)
    per_layer = grads.shape[0] // layers
    pieces = [(layer, i) for layer in range(layers) for i in range(3)]

    def own(ref, layer, i):
        rows = m_in[i].shape[1]
        return ref.at[layer, pl.ds(pl.multiple_of(me * rows, 8), rows), :]

    loads = []
    for p, (layer, i) in enumerate(pieces):
        loads.append(
            [
                pltpu.make_async_copy(own(w_h[i], layer, i), w_in[i].at[layer], load_sem.at[p, 0]),
                pltpu.make_async_copy(m_h[i].at[layer], m_in[i].at[layer], load_sem.at[p, 1]),
                pltpu.make_async_copy(v_h[i].at[layer], v_in[i].at[layer], load_sem.at[p, 2]),
            ]
        )
        for one in loads[-1]:
            one.start()
    everyone[me] = jnp.sum(squares[...].reshape(-1, 8, LANES), axis=0)
    enter([lax.rem(me + i, n) for i in range(1, n)])
    shares = []
    for i in range(1, n):
        shares.append(
            pltpu.make_async_remote_copy(
                src_ref=everyone.at[me],
                dst_ref=everyone.at[me],
                send_sem=s_send.at[i - 1],
                recv_sem=s_recv.at[i - 1],
                device_id={"dp": lax.rem(me + i, n)},
                device_id_type=MESH,
            )
        )
        shares[-1].start()
    for i in range(1, n):
        source = lax.rem(me + n - i, n)
        pltpu.make_async_remote_copy(
            src_ref=everyone.at[source],
            dst_ref=everyone.at[source],
            send_sem=s_send.at[i - 1],
            recv_sem=s_recv.at[i - 1],
            device_id={"dp": lax.rem(me + i, n)},
            device_id_type=MESH,
        ).wait_recv()
    square = jnp.sum(everyone[...])
    factor = jnp.minimum(1.0, 0.5 * lax.rsqrt(square / count + 1e-30))

    def step(w, m, v, g):
        g = g.astype(F32) * factor
        m = 0.9 * m + 0.1 * g
        v = 0.95 * v + 0.05 * g * g
        w = w.astype(F32)
        return (w - 0.02 * (m * lax.rsqrt(v + 1e-8) + 0.1 * w)).astype(BF), m, v

    def block(ref, p, chip, core, part=None):
        layer, i = pieces[p]
        rows, cols = m_in[i].shape[1:]
        start = (chip * 2 + core) * rows
        if part is None:
            return ref.at[layer, pl.ds(pl.multiple_of(start, 8), rows), :]
        if i == 2:
            return ref.at[layer, pl.ds(pl.multiple_of(start + part * (rows // 2), 8), rows // 2), :]
        return ref.at[layer, pl.ds(pl.multiple_of(start, 8), rows), pl.ds(part * (cols // 2), cols // 2)]

    def part_of(ref, p, part):
        layer, i = pieces[p]
        rows, cols = m_in[i].shape[1:]
        if i == 2:
            return ref.at[layer, pl.ds(part * (rows // 2), rows // 2), :]
        return ref.at[layer, :, pl.ds(part * (cols // 2), cols // 2)]

    def hop(way, s, p):
        i = pieces[p][1]
        chip = lax.rem(z + (chips - s if way == 0 else s), chips)
        part = way if s == half - 1 else None
        dst = block(w_out[i], p, chip, c, part)
        if s == 0:
            src = w_in[i].at[pieces[p][0]] if part is None else part_of(w_in[i], p, part)
        else:
            src = dst
        return pltpu.make_async_remote_copy(
            src_ref=src,
            dst_ref=dst,
            send_sem=r_send.at[way, s, p],
            recv_sem=r_recv.at[way, s, p],
            device_id={"dp": plus if way == 0 else minus},
            device_id_type=MESH,
        )

    def across(j, p):
        i = pieces[p][1]
        if j == 0:
            src, dst = w_in[i].at[pieces[p][0]], block(w_out[i], p, z, c)
        else:
            s, way = (j - 1) // 2, (j - 1) % 2
            chip = lax.rem(z + (chips - 1 - s if way == 0 else 1 + s), chips)
            dst = block(w_out[i], p, chip, c, way if s == half - 1 else None)
            src = dst
        return pltpu.make_async_remote_copy(
            src_ref=src,
            dst_ref=dst,
            send_sem=d_send.at[j, p],
            recv_sem=d_recv.at[j, p],
            device_id={"dp": partner},
            device_id_type=MESH,
        )

    stores = []
    for p, (layer, i) in enumerate(pieces):
        for one in loads[p]:
            one.wait()
        base = (layers - 1 - layer) * per_layer
        rows, cols = m_in[i].shape[1:]
        w1, m1, v1 = w_in[i], m_in[i], v_in[i]
        if i < 2:

            def column(q, _, base=base, layer=layer, i=i, w1=w1, m1=m1, v1=v1):
                t, r = q // QUARTERS, lax.rem(q, QUARTERS)
                at_cols = pl.ds(pl.multiple_of(q * LANES, LANES), LANES)
                g = grads[base + t * QUARTERS + 2 * i + r // 2, lax.rem(r, 2)]
                w, m, v = step(w1[layer, :, at_cols], m1[layer, :, at_cols], v1[layer, :, at_cols], g)
                w1[layer, :, at_cols] = w
                m1[layer, :, at_cols] = m
                v1[layer, :, at_cols] = v
                return 0

            lax.fori_loop(0, cols // LANES, column, 0)
        else:

            def row(j, _, base=base, layer=layer, w1=w1, m1=m1, v1=v1):
                at_rows = pl.ds(pl.multiple_of(j * 16, 16), 16)
                g = grads[base + tiles * QUARTERS + j].astype(F32)
                g = jnp.concatenate(
                    [jnp.concatenate([g[r, 8 * q : 8 * q + 8, :] for q in range(cols // LANES)], axis=1) for r in (0, 1)], axis=0
                )
                w, m, v = step(w1[layer, at_rows, :], m1[layer, at_rows, :], v1[layer, at_rows, :], g)
                w1[layer, at_rows, :] = w
                m1[layer, at_rows, :] = m
                v1[layer, at_rows, :] = v
                return 0

            lax.fori_loop(0, rows // 16, row, 0)
        stores.append(pltpu.make_async_copy(m1.at[layer], m_out[i].at[layer], store_sem.at[p, 0]))
        stores.append(pltpu.make_async_copy(v1.at[layer], v_out[i].at[layer], store_sem.at[p, 1]))
        stores.append(pltpu.make_async_copy(w1.at[layer], block(w_out[i], p, z, c), store_sem.at[p, 2]))
        for way in (0, 1):
            hop(way, 0, p).start()
        across(0, p).start()
        for one in stores[-3:]:
            one.start()
    for s in range(1, half + 1):
        for p in range(len(pieces)):
            for way in (0, 1):
                hop(way, s - 1, p).wait_recv()
                if s < half:
                    hop(way, s, p).start()
                across(1 + 2 * (s - 1) + way, p).start()
    for one in stores:
        one.wait()
    for p in range(len(pieces)):
        for j in range(1 + 2 * half):
            across(j, p).wait()
        for s in range(half):
            for way in (0, 1):
                hop(way, s, p).wait_send()
    for one in shares:
        one.wait_send()


def update(n, grads, squares, ws, ms, vs):
    layers, d, ff = ws[0].shape
    half = n // 4
    pieces = 3 * layers
    tiles = ff // TILE
    hbm, vmem = pl.BlockSpec(memory_space=pl.ANY), pl.BlockSpec(memory_space=pltpu.VMEM)
    count = sum(w.size for w in ws)
    like = lambda t, dt=None: jax.ShapeDtypeStruct(t.shape, dt or t.dtype)
    return pl.pallas_call(
        functools.partial(update_kernel, n, layers, tiles, count),
        in_specs=[vmem, vmem] + [hbm] * 9,
        out_specs=[hbm] * 9,
        out_shape=[like(t) for t in (*ws, *ms, *vs)],
        scratch_shapes=[pltpu.VMEM(m.shape, BF) for m in ms]
        + [pltpu.VMEM(m.shape, F32) for m in ms]
        + [pltpu.VMEM(v.shape, F32) for v in vs]
        + [
            pltpu.VMEM((n, 8, LANES), F32),
            pltpu.SemaphoreType.DMA((pieces, 3)),
            pltpu.SemaphoreType.DMA((pieces, 3)),
            pltpu.SemaphoreType.DMA((n - 1,)),
            pltpu.SemaphoreType.DMA((n - 1,)),
            pltpu.SemaphoreType.DMA((2, half, pieces)),
            pltpu.SemaphoreType.DMA((2, half, pieces)),
            pltpu.SemaphoreType.DMA((1 + 2 * half, pieces)),
            pltpu.SemaphoreType.DMA((1 + 2 * half, pieces)),
        ],
        compiler_params=pltpu.CompilerParams(collective_id=1, has_side_effects=True, vmem_limit_bytes=40_000_000),
        name="update",
    )(grads, squares, *ws, *ms, *vs)


def solution(mesh):
    n = mesh.shape["dp"]

    def of_a_device(x, dy, *arrays):
        ws, ms, vs = (arrays[i : i + 3] for i in (0, 3, 6))
        a0, at0, h1, a1, at1 = forward(x[0], *ws, 0)
        grads, squares = backward(n, a0, at0, a1, at1, h1, dy[0], *ws)
        return tuple(update(n, grads, squares, ws, ms, vs))

    seq, whole, rows = P(("rep", "dp")), P(), P(None, "dp")
    return jax.shard_map(
        of_a_device,
        mesh=mesh,
        in_specs=(seq, seq) + (whole,) * 3 + (rows,) * 6,
        out_specs=(P("rep"),) * 3 + (P("rep", "dp"),) * 6,
        check_vma=False,
    )
```

```python
import functools

import jax
import jax.numpy as jnp
from jax import lax
from jax.experimental import pallas as pl
from jax.experimental.pallas import tpu as pltpu
from jax.sharding import PartitionSpec as P

MESH = pl.DeviceIdType.MESH
BF, F32 = jnp.bfloat16, jnp.float32
LANES = 128
TILE = 512
QUARTERS = TILE // LANES
ROWS = 256
LAG = 2
LAG_PARTNER = 1
RING_GRAD, RING_SUM, RING_PARTNER = 4, 10, 4
VMEM_LIMIT = 62_000_000


def nn(a, b):
    return lax.dot_general(a, b, (((1,), (0,)), ((), ())), preferred_element_type=F32)


def nt(a, b):
    return lax.dot_general(a, b, (((1,), (1,)), ((), ())), preferred_element_type=F32)


def tn(a, b):
    return lax.dot_general(a, b, (((0,), (0,)), ((), ())), preferred_element_type=F32)


def normed(h):
    wide = h.astype(F32)
    scale = lax.rsqrt(jnp.mean(wide * wide, -1, keepdims=True) + 1e-6)
    return (wide * scale).astype(BF)


def sigmoid(x):
    return 1.0 / (1.0 + jnp.exp(-x))


def places(n):
    me = lax.axis_index("dp")
    chips = n // 2
    z, c = me // 2, lax.rem(me, 2)
    plus = lax.rem(z + 1, chips) * 2 + c
    minus = lax.rem(z + chips - 1, chips) * 2 + c
    return me, z, c, z * 2 + 1 - c, plus, minus


def greet(others):
    for o in others:
        pl.semaphore_signal(pltpu.get_barrier_semaphore(), inc=1, device_id={"dp": o}, device_id_type=MESH)


def meet(count):
    pl.semaphore_wait(pltpu.get_barrier_semaphore(), count)


def backward_kernel(
    n, layers, tiles, rows,
    x_h, dy_h, wg_h, wu_h, wd_h,
    out, square,
    h, a0, a1, at, dy, wg, wu, wd, act, dgate, dup, acc,
    grad, partner_sum, total, hop_in, squares, everyone,
    d_send, d_recv, r_send, r_recv, s_send, s_recv, load_sem, wide_sem, tall_sem,
):
    chips, half = n // 2, n // 4
    per_layer = 3 * tiles
    chunks = layers * per_layer
    slots = 2 * LAG
    full = LAG_PARTNER + LAG * half
    me, z, c, partner, plus, minus = places(n)
    tokens, d = h.shape

    def wide_weight(i, layer, t):
        w_h, w = ((wg_h, wg), (wu_h, wu))[i]
        at_tile = pl.ds(pl.multiple_of(t * TILE, TILE), TILE)
        return pltpu.make_async_copy(w_h.at[layer, :, at_tile], w.at[t], wide_sem.at[i, t])

    def wide_weights(layer, t):
        return [wide_weight(i, layer, t) for i in (0, 1)]

    def tall_weights(layer, t, turn):
        b = lax.rem(turn, 2)
        at_tile = pl.ds(pl.multiple_of(t * TILE, TILE), TILE)
        return pltpu.make_async_copy(wd_h.at[layer, at_tile, :], wd.at[b], tall_sem.at[b])

    def each_tile(what):
        def body(t, _):
            what(t)
            return 0

        lax.fori_loop(0, tiles, body, 0)

    def start(copies):
        for one in copies:
            one.start()

    def wait(copies):
        for one in copies:
            one.wait()

    def next_tall(layer, t, turn, after):
        tall_weights(layer, t, turn).wait()

        @pl.when(t + 1 < tiles)
        def _():
            tall_weights(layer, t + 1, turn + 1).start()

        if after is not None:

            @pl.when(t + 1 == tiles)
            def _():
                tall_weights(after, jnp.int32(0), turn + 1).start()

    load_x = pltpu.make_async_copy(x_h, h, load_sem.at[0])
    load_dy = pltpu.make_async_copy(dy_h, dy, load_sem.at[1])
    load_x.start()
    start(wide_weights(0, jnp.int32(0)))
    tall_weights(0, jnp.int32(0), jnp.int32(0)).start()
    for t in range(1, tiles):
        start(wide_weights(0, jnp.int32(t)))
    load_dy.start()
    others = [lax.rem(me + i, n) for i in range(1, n)]
    greet(others)
    squares[...] = jnp.zeros_like(squares)
    acc[...] = jnp.zeros_like(acc)

    def place_of(k):
        within = lax.rem(k, per_layer)
        tall = within // (2 * tiles)
        return tall * (within - 2 * tiles + RING_GRAD) + (1 - tall) * lax.rem(within, RING_GRAD)

    def to_partner(k):
        b = lax.rem(k, RING_PARTNER)
        return pltpu.make_async_remote_copy(
            src_ref=grad.at[place_of(k), 1 - c],
            dst_ref=partner_sum.at[b],
            send_sem=d_send.at[b],
            recv_sem=d_recv.at[b],
            device_id={"dp": partner},
            device_id_type=MESH,
        )

    def target(way, s):
        return lax.rem(z + (half - s if way == 0 else chips - half + s), chips)

    def hop(way, s, slot):
        k = lax.rem(slot - LAG_PARTNER - LAG * s, RING_SUM)
        b = lax.rem(slot, slots)
        src, dst = total.at[k, target(way, s)], hop_in.at[way, s, b]
        if s == 0:
            src, dst = src.at[way], dst.at[way]
        return pltpu.make_async_remote_copy(
            src_ref=src,
            dst_ref=dst,
            send_sem=r_send.at[way, s, b],
            recv_sem=r_recv.at[way, s, b],
            device_id={"dp": plus if way == 0 else minus},
            device_id_type=MESH,
        )

    def add_partner(k):
        i, g, b = lax.rem(k, RING_SUM), place_of(k), lax.rem(k, RING_PARTNER)
        for j in range(chips):
            total[i, j] = (grad[g, c, j].astype(F32) + partner_sum[b, j].astype(F32)).astype(BF)

    def add_hop(way, s, k, now):
        i, b, far = lax.rem(k, RING_SUM), lax.rem(now - LAG, slots), target(way, s)
        if s == 1:
            total[i, far, way] = (total[i, far, way].astype(F32) + hop_in[way, 0, b, way].astype(F32)).astype(BF)
        else:
            total[i, far] = (total[i, far].astype(F32) + hop_in[way, s - 1, b].astype(F32)).astype(BF)

    def finish(k, now):
        b = lax.rem(now - LAG, slots)
        own = total[lax.rem(k, RING_SUM), z].astype(F32)
        g = (own + hop_in[0, half - 1, b].astype(F32) + hop_in[1, half - 1, b].astype(F32)).astype(BF)
        out[k] = g
        wide = g.astype(F32)
        squares[...] += wide[0, 0] * wide[0, 0] + wide[0, 1] * wide[0, 1] + wide[1, 0] * wide[1, 0] + wide[1, 1] * wide[1, 1]

    def slot(now):
        ks = [now - LAG_PARTNER - LAG * s for s in range(half + 1)]
        filled = (ks[half] >= 0) & (now < chunks)

        @pl.when(filled)
        def _():
            to_partner(now).start()
            to_partner(ks[0]).wait()
            for s in range(1, half + 1):
                for way in (0, 1):
                    hop(way, s - 1, now - LAG).wait()
            add_partner(ks[0])
            for s in range(1, half):
                for way in (0, 1):
                    add_hop(way, s, ks[s], now)
            finish(ks[half], now)
            for s in range(half):
                for way in (0, 1):
                    hop(way, s, now).start()

        @pl.when(jnp.logical_not(filled))
        def _():
            def during(k):
                return (k >= 0) & (k < chunks)

            @pl.when(during(now))
            def _():
                to_partner(now).start()

            @pl.when(during(ks[0]))
            def _():
                to_partner(ks[0]).wait()
                add_partner(ks[0])

            for s in range(1, half + 1):

                @pl.when(during(ks[s]))
                def _(s=s):
                    for way in (0, 1):
                        hop(way, s - 1, now - LAG).wait()
                    if s < half:
                        for way in (0, 1):
                            add_hop(way, s, ks[s], now)
                    else:
                        finish(ks[s], now)

            for s in range(half):

                @pl.when(during(ks[s]))
                def _(s=s):
                    for way in (0, 1):
                        hop(way, s, now).start()

    def forward(b, a, t):
        for r in range(0, tokens, ROWS):
            mine = a[r : r + ROWS, :]
            gate = nn(mine, wg[t])
            up = nn(mine, wu[t])
            hidden = (gate * sigmoid(gate) * up).astype(BF)
            acc[r : r + ROWS, :] += nn(hidden, wd[b])

    def elementwise(b, a, t):
        for r in range(0, tokens, ROWS):
            at_rows = pl.ds(r, ROWS)
            gate = nn(a[at_rows, :], wg[t])
            up = nn(a[at_rows, :], wu[t])
            by_act = nt(dy[at_rows, :], wd[b]).astype(BF).astype(F32)
            s = sigmoid(gate)
            silu = gate * s
            act[t, at_rows, :] = (silu * up).astype(BF)
            dup[t, at_rows, :] = (by_act * silu).astype(BF)
            dgate[t, at_rows, :] = (by_act * up * (s * (1.0 + gate * (1.0 - s)))).astype(BF)

    def wide_grad(source, chunk, t):
        k = place_of(chunk)
        for p in range(2):
            g = nn(at[p * (d // 2) : (p + 1) * (d // 2), :], source[t])
            for i in range(n // 2):
                dev = p * (n // 2) + i
                for q in range(QUARTERS):
                    grad[k, dev % 2, dev // 2, q // 2, q % 2] = g[i * rows : (i + 1) * rows, q * LANES : (q + 1) * LANES].astype(BF)

    def tall_grad(t):
        acc[:TILE, :] = tn(act[t], dy[...])
        per_dev = tiles * TILE // n // 8

        def group(i, _):
            g = t * (TILE // 8) + i
            dev, rest = g // per_dev, lax.rem(g, per_dev)
            k = RING_GRAD + rest // 4
            eight = acc[pl.ds(pl.multiple_of(i * 8, 8), 8), :]
            stacked = jnp.concatenate([eight[:, q * LANES : (q + 1) * LANES] for q in range(d // LANES)], axis=0)
            quarter = lax.rem(rest, 4)
            grad[k, lax.rem(dev, 2), dev // 2, quarter // 2, lax.rem(quarter, 2)] = stacked.astype(BF)
            return 0

        lax.fori_loop(0, TILE // 8, group, 0, unroll=8)

    def to_states(layer, a, first_slot):
        turn = 0
        for source, w, w_h in ((dgate, wg, wg_h), (dup, wu, wu_h)):
            for r in range(0, tokens, tokens // 2):
                at_rows = pl.ds(r, tokens // 2)
                part = nt(source[0, at_rows, :], w[0])
                for t in range(1, tiles):
                    part += nt(source[t, at_rows, :], w[t])
                if source is dgate:
                    a[at_rows, :] = part.astype(BF)
                else:
                    acc[at_rows, :] = part
                slot(first_slot + turn)
                turn += 1
            which = 0 if source is dgate else 1
            for t in range(tiles):
                wide_weight(which, layer - 1, jnp.int32(t)).start()

        def norm(i, _):
            at_rows = pl.ds(pl.multiple_of(i * 64, 64), 64)
            by_a = (a[at_rows, :].astype(F32) + acc[at_rows, :].astype(BF).astype(F32)).astype(BF).astype(F32)
            wide = h[at_rows, :].astype(F32)
            scale = lax.rsqrt(jnp.mean(wide * wide, -1, keepdims=True) + 1e-6)
            along = jnp.mean(by_a * wide, -1, keepdims=True)
            by_h = (by_a * scale - wide * (scale * scale * scale * along)).astype(BF)
            dy[at_rows, :] = (dy[at_rows, :].astype(F32) + by_h.astype(F32)).astype(BF)
            return 0

        lax.fori_loop(0, tokens // 64, norm, 0)
        slot(first_slot + turn)

    load_x.wait()
    for r in range(0, tokens, 128):
        a0[r : r + 128, :] = normed(h[r : r + 128, :])

    def ahead(t):
        wait(wide_weights(0, t))
        next_tall(0, t, t, layers - 1)
        forward(lax.rem(t, 2), a0, t)
        start(wide_weights(layers - 1, t))

    each_tile(ahead)
    for r in range(0, tokens, 128):
        new = (h[r : r + 128, :].astype(F32) + acc[r : r + 128, :].astype(BF).astype(F32)).astype(BF)
        h[r : r + 128, :] = new
        a1[r : r + 128, :] = normed(new)
    at[...] = a1[...].T
    load_dy.wait()
    meet(n - 1)

    for step in range(layers):
        layer = layers - 1 - step
        base = step * per_layer
        a = (a0, a1)[layer]

        def tile(t, layer=layer, base=base, a=a, step=step):
            turn = (step + 1) * tiles + t
            wait(wide_weights(layer, t))
            next_tall(layer, t, turn, layer - 1 if layer > 0 else None)
            chunk = base + 2 * t
            elementwise(lax.rem(turn, 2), a, t)
            slot(chunk - 1)
            wide_grad(dgate, chunk, t)
            slot(chunk)
            wide_grad(dup, chunk + 1, t)
            tall_grad(t)

        each_tile(tile)
        if step < layers - 1:
            to_states(layer, a, base + 2 * tiles - 1)
            at[...] = a0[...].T

    def rest(i, _):
        slot(i)
        return 0

    lax.fori_loop((layers - 1) * per_layer + 2 * tiles - 1, chunks + full, rest, 0)

    everyone[me] = jnp.sum(squares[...].reshape(-1, 8, LANES), axis=0)

    def share(i, source):
        return pltpu.make_async_remote_copy(
            src_ref=everyone.at[source],
            dst_ref=everyone.at[source],
            send_sem=s_send.at[i],
            recv_sem=s_recv.at[i],
            device_id={"dp": others[i]},
            device_id_type=MESH,
        )

    for i in range(n - 1):
        share(i, me).start()
    for i in range(n - 1):
        share(i, lax.rem(me + n - 1 - i, n)).wait_recv()
    square[...] = jnp.sum(everyone[...], axis=0)
    for i in range(n - 1):
        share(i, me).wait_send()


def backward(n, x, dy, wg, wu, wd):
    layers, d, ff = wg.shape
    tokens = dy.shape[0]
    tiles, rows, chips, half = ff // TILE, d // n, n // 2, n // 4
    chunks = 3 * layers * tiles
    unit = (2, 2, rows, LANES)
    hbm, vmem = pl.BlockSpec(memory_space=pl.ANY), pl.BlockSpec(memory_space=pltpu.VMEM)
    return pl.pallas_call(
        functools.partial(backward_kernel, n, layers, tiles, rows),
        in_specs=[hbm] * 5,
        out_specs=[vmem] * 2,
        out_shape=[pltpu.VMEM((chunks,) + unit, BF), pltpu.VMEM((8, LANES), F32)],
        scratch_shapes=[
            pltpu.VMEM((tokens, d), BF),
            pltpu.VMEM((tokens, d), BF),
            pltpu.VMEM((tokens, d), BF),
            pltpu.VMEM((d, tokens), BF),
            pltpu.VMEM((tokens, d), BF),
            pltpu.VMEM((tiles, d, TILE), BF),
            pltpu.VMEM((tiles, d, TILE), BF),
            pltpu.VMEM((2, TILE, d), BF),
            pltpu.VMEM((tiles, tokens, TILE), BF),
            pltpu.VMEM((tiles, tokens, TILE), BF),
            pltpu.VMEM((tiles, tokens, TILE), BF),
            pltpu.VMEM((tokens, d), F32),
            pltpu.VMEM((RING_GRAD + tiles, 2, chips) + unit, BF),
            pltpu.VMEM((RING_PARTNER, chips) + unit, BF),
            pltpu.VMEM((RING_SUM, chips) + unit, BF),
            pltpu.VMEM((2, half, 2 * LAG) + unit, BF),
            pltpu.VMEM((rows, LANES), F32),
            pltpu.VMEM((n, 8, LANES), F32),
            pltpu.SemaphoreType.DMA((RING_PARTNER,)),
            pltpu.SemaphoreType.DMA((RING_PARTNER,)),
            pltpu.SemaphoreType.DMA((2, half, 2 * LAG)),
            pltpu.SemaphoreType.DMA((2, half, 2 * LAG)),
            pltpu.SemaphoreType.DMA((n - 1,)),
            pltpu.SemaphoreType.DMA((n - 1,)),
            pltpu.SemaphoreType.DMA((2,)),
            pltpu.SemaphoreType.DMA((2, tiles)),
            pltpu.SemaphoreType.DMA((2,)),
        ],
        compiler_params=pltpu.CompilerParams(collective_id=0, has_side_effects=True, vmem_limit_bytes=VMEM_LIMIT),
        name="backward",
    )(x, dy, wg, wu, wd)


def update_kernel(n, layers, tiles, count, *refs):
    grads, square = refs[:2]
    w_h, m_h, v_h = refs[2:5], refs[5:8], refs[8:11]
    w_out, m_in, v_in = refs[11:14], refs[14:17], refs[17:20]
    w_in = refs[20:23]
    load_sem, r_send, r_recv, d_send, d_recv = refs[23:]
    chips, half = n // 2, n // 4
    me, z, c, partner, plus, minus = places(n)
    per_layer = grads.shape[0] // layers
    pieces = [(layer, i) for layer in range(layers) for i in range(3)]

    def own(ref, layer, i):
        rows = m_in[i].shape[1]
        return ref.at[layer, pl.ds(pl.multiple_of(me * rows, 8), rows), :]

    loads = []
    for p, (layer, i) in enumerate(pieces):
        loads.append(
            [
                pltpu.make_async_copy(own(w_h[i], layer, i), w_in[i].at[layer], load_sem.at[p, 0]),
                pltpu.make_async_copy(m_h[i].at[layer], m_in[i].at[layer], load_sem.at[p, 1]),
                pltpu.make_async_copy(v_h[i].at[layer], v_in[i].at[layer], load_sem.at[p, 2]),
            ]
        )
        for one in loads[-1]:
            one.start()
    greet([partner, plus, minus])
    factor = jnp.minimum(1.0, 0.5 * lax.rsqrt(jnp.sum(square[...]) / count + 1e-30))

    def step(w, m, v, g):
        g = g.astype(F32) * factor
        m = 0.9 * m + 0.1 * g
        v = 0.95 * v + 0.05 * g * g
        w = w.astype(F32)
        return (w - 0.02 * (m * lax.rsqrt(v + 1e-8) + 0.1 * w)).astype(BF), m, v

    def block(ref, p, chip, core, part=None):
        layer, i = pieces[p]
        rows, cols = m_in[i].shape[1:]
        start = (chip * 2 + core) * rows
        if part is None:
            return ref.at[layer, pl.ds(pl.multiple_of(start, 8), rows), :]
        if i == 2:
            return ref.at[layer, pl.ds(pl.multiple_of(start + part * (rows // 2), 8), rows // 2), :]
        return ref.at[layer, pl.ds(pl.multiple_of(start, 8), rows), pl.ds(part * (cols // 2), cols // 2)]

    def part_of(ref, p, part):
        layer, i = pieces[p]
        rows, cols = m_in[i].shape[1:]
        if i == 2:
            return ref.at[layer, pl.ds(part * (rows // 2), rows // 2), :]
        return ref.at[layer, :, pl.ds(part * (cols // 2), cols // 2)]

    def hop(way, s, p):
        i = pieces[p][1]
        chip = lax.rem(z + (chips - s if way == 0 else s), chips)
        part = way if s == half - 1 else None
        dst = block(w_out[i], p, chip, c, part)
        if s == 0:
            src = w_in[i].at[pieces[p][0]] if part is None else part_of(w_in[i], p, part)
        else:
            src = dst
        return pltpu.make_async_remote_copy(
            src_ref=src,
            dst_ref=dst,
            send_sem=r_send.at[way, s, p],
            recv_sem=r_recv.at[way, s, p],
            device_id={"dp": plus if way == 0 else minus},
            device_id_type=MESH,
        )

    def across(j, p):
        i = pieces[p][1]
        if j == 0:
            src, dst = w_in[i].at[pieces[p][0]], block(w_out[i], p, z, c)
        else:
            s, way = (j - 1) // 2, (j - 1) % 2
            chip = lax.rem(z + (chips - 1 - s if way == 0 else 1 + s), chips)
            dst = block(w_out[i], p, chip, c, way if s == half - 1 else None)
            src = dst
        return pltpu.make_async_remote_copy(
            src_ref=src,
            dst_ref=dst,
            send_sem=d_send.at[j, p],
            recv_sem=d_recv.at[j, p],
            device_id={"dp": partner},
            device_id_type=MESH,
        )

    for p, (layer, i) in enumerate(pieces):
        for one in loads[p]:
            one.wait()
        base = (layers - 1 - layer) * per_layer
        rows, cols = m_in[i].shape[1:]
        w1, m1, v1 = w_in[i], m_in[i], v_in[i]
        if i < 2:

            def column(q, _, base=base, layer=layer, i=i, w1=w1, m1=m1, v1=v1):
                t, r = q // QUARTERS, lax.rem(q, QUARTERS)
                at_cols = pl.ds(pl.multiple_of(q * LANES, LANES), LANES)
                g = grads[base + 2 * t + i, r // 2, lax.rem(r, 2)]
                w, m, v = step(w1[layer, :, at_cols], m1[layer, :, at_cols], v1[layer, :, at_cols], g)
                w1[layer, :, at_cols] = w
                m1[layer, :, at_cols] = m
                v1[layer, :, at_cols] = v
                return 0

            lax.fori_loop(0, cols // LANES, column, 0, unroll=5)
        else:

            def row(j, _, base=base, layer=layer, w1=w1, m1=m1, v1=v1):
                at_rows = pl.ds(pl.multiple_of(j * 32, 32), 32)
                g = grads[base + 2 * tiles + j].astype(F32)
                eights = [g[r // 2, r % 2] for r in range(4)]
                g = jnp.concatenate(
                    [jnp.concatenate([e[8 * q : 8 * q + 8, :] for q in range(cols // LANES)], axis=1) for e in eights], axis=0
                )
                w, m, v = step(w1[layer, at_rows, :], m1[layer, at_rows, :], v1[layer, at_rows, :], g)
                w1[layer, at_rows, :] = w
                m1[layer, at_rows, :] = m
                v1[layer, at_rows, :] = v
                return 0

            lax.fori_loop(0, rows // 32, row, 0, unroll=5)
        if p == 0:
            meet(3)
        for way in (0, 1):
            hop(way, 0, p).start()
        across(0, p).start()
        start = pl.ds(pl.multiple_of(me * rows, 8), rows)
        w_out[i][layer, start, :] = w1[layer]
    for s in range(1, half + 1):
        for p in range(len(pieces)):
            for way in (0, 1):
                hop(way, s - 1, p).wait_recv()
                if s < half:
                    hop(way, s, p).start()
                across(1 + 2 * (s - 1) + way, p).start()
    for p in range(len(pieces)):
        for j in range(1 + 2 * half):
            across(j, p).wait()
        for s in range(half):
            for way in (0, 1):
                hop(way, s, p).wait_send()


def update(n, grads, square, ws, ms, vs):
    layers, d, ff = ws[0].shape
    half = n // 4
    pieces = 3 * layers
    tiles = ff // TILE
    hbm, vmem = pl.BlockSpec(memory_space=pl.ANY), pl.BlockSpec(memory_space=pltpu.VMEM)
    count = sum(w.size for w in ws)
    like = lambda t, dt=None: jax.ShapeDtypeStruct(t.shape, dt or t.dtype)
    return pl.pallas_call(
        functools.partial(update_kernel, n, layers, tiles, count),
        in_specs=[vmem, vmem] + [hbm] * 9,
        out_specs=[vmem] * 9,
        out_shape=[pltpu.VMEM(t.shape, t.dtype) for t in (*ws, *ms, *vs)],
        scratch_shapes=[pltpu.VMEM(m.shape, BF) for m in ms]
        + [
            pltpu.SemaphoreType.DMA((pieces, 3)),
            pltpu.SemaphoreType.DMA((2, half, pieces)),
            pltpu.SemaphoreType.DMA((2, half, pieces)),
            pltpu.SemaphoreType.DMA((1 + 2 * half, pieces)),
            pltpu.SemaphoreType.DMA((1 + 2 * half, pieces)),
        ],
        compiler_params=pltpu.CompilerParams(collective_id=1, has_side_effects=True, vmem_limit_bytes=4_000_000),
        name="update",
    )(
        *(pltpu.with_memory_space_constraint(t, pltpu.VMEM) for t in (grads, square)),
        *(pltpu.with_memory_space_constraint(t, pltpu.HBM) for t in (*ws, *ms, *vs)),
    )


def place_kernel(*refs):
    k = len(refs) // 2
    sems = refs[-1]
    copies = [pltpu.make_async_copy(refs[i], refs[k + i], sems.at[i]) for i in range(k)]
    for one in copies:
        one.start()
    for one in copies:
        one.wait()


def place(arrays):
    hbm, vmem = pl.BlockSpec(memory_space=pl.ANY), pl.BlockSpec(memory_space=pltpu.VMEM)
    return pl.pallas_call(
        place_kernel,
        in_specs=[vmem] * len(arrays),
        out_specs=[hbm] * len(arrays),
        out_shape=[pltpu.HBM(t.shape, t.dtype) for t in arrays],
        scratch_shapes=[pltpu.SemaphoreType.DMA((len(arrays),))],
        compiler_params=pltpu.CompilerParams(vmem_limit_bytes=1_000_000),
        name="place",
    )(*(pltpu.with_memory_space_constraint(t, pltpu.VMEM) for t in arrays))


def solution(mesh):
    n = mesh.shape["dp"]

    def of_a_device(x, dy, *arrays):
        ws, ms, vs = (arrays[i : i + 3] for i in (0, 3, 6))
        grads, square = backward(n, x[0], dy[0], *ws)
        return tuple(place(update(n, grads, square, ws, ms, vs)))

    seq, whole, rows = P(("rep", "dp")), P(), P(None, "dp")
    return jax.shard_map(
        of_a_device,
        mesh=mesh,
        in_specs=(seq, seq) + (whole,) * 3 + (rows,) * 6,
        out_specs=(P("rep"),) * 3 + (P("rep", "dp"),) * 6,
        check_vma=False,
    )
```

```python
import functools

import jax
import jax.numpy as jnp
from jax import lax
from jax.experimental import pallas as pl
from jax.experimental.pallas import tpu as pltpu
from jax.sharding import PartitionSpec as P

MESH = pl.DeviceIdType.MESH
BF, F32 = jnp.bfloat16, jnp.float32
LANES = 128
TILE = 512
QUARTERS = TILE // LANES
ROWS = 256
LAG = 2
LAG_PARTNER = 1
RING_GRAD, RING_SUM, RING_PARTNER = 4, 10, 4
VMEM_LIMIT = 63_500_000


def nn(a, b):
    return lax.dot_general(a, b, (((1,), (0,)), ((), ())), preferred_element_type=F32)


def nt(a, b):
    return lax.dot_general(a, b, (((1,), (1,)), ((), ())), preferred_element_type=F32)


def tn(a, b):
    return lax.dot_general(a, b, (((0,), (0,)), ((), ())), preferred_element_type=F32)


def normed(h):
    wide = h.astype(F32)
    scale = lax.rsqrt(jnp.mean(wide * wide, -1, keepdims=True) + 1e-6)
    return (wide * scale).astype(BF)


def sigmoid(x):
    return 1.0 / (1.0 + jnp.exp(-x))


def places(n):
    me = lax.axis_index("dp")
    chips = n // 2
    z, c = me // 2, lax.rem(me, 2)
    plus = lax.rem(z + 1, chips) * 2 + c
    minus = lax.rem(z + chips - 1, chips) * 2 + c
    return me, z, c, z * 2 + 1 - c, plus, minus


def greet(others):
    for o in others:
        pl.semaphore_signal(pltpu.get_barrier_semaphore(), inc=1, device_id={"dp": o}, device_id_type=MESH)


def meet(count):
    pl.semaphore_wait(pltpu.get_barrier_semaphore(), count)


def backward_kernel(
    n, layers, tiles, rows,
    x_h, dy_h, wg_h, wu_h, wd_h, m_h, v_h,
    out, square, w_first, m_first, v_first,
    h, a0, a1, at, dy, wg, wu, wd, act, dgate, dup, acc,
    grad, partner_sum, total, hop_out, hop_in, squares, everyone,
    d_send, d_recv, r_send, r_recv, s_send, s_recv, load_sem, wide_sem, tall_sem,
):
    chips, half = n // 2, n // 4
    per_layer = 3 * tiles
    chunks = layers * per_layer
    slots = 2 * LAG
    full = LAG_PARTNER + LAG * half
    me, z, c, partner, plus, minus = places(n)
    tokens, d = h.shape

    def wide_weight(i, layer, t):
        w_h, w = ((wg_h, wg), (wu_h, wu))[i]
        at_tile = pl.ds(pl.multiple_of(t * TILE, TILE), TILE)
        return pltpu.make_async_copy(w_h.at[layer, :, at_tile], w.at[t], wide_sem.at[i, t])

    def wide_weights(layer, t):
        return [wide_weight(i, layer, t) for i in (0, 1)]

    def tall_weights(layer, t, turn):
        b = lax.rem(turn, 2)
        at_tile = pl.ds(pl.multiple_of(t * TILE, TILE), TILE)
        return pltpu.make_async_copy(wd_h.at[layer, at_tile, :], wd.at[b], tall_sem.at[b])

    def each_tile(what):
        def body(t, _):
            what(t)
            return 0

        lax.fori_loop(0, tiles, body, 0)

    def start(copies):
        for one in copies:
            one.start()

    def wait(copies):
        for one in copies:
            one.wait()

    def next_tall(layer, t, turn, after):
        tall_weights(layer, t, turn).wait()

        @pl.when(t + 1 < tiles)
        def _():
            tall_weights(layer, t + 1, turn + 1).start()

        if after is not None:

            @pl.when(t + 1 == tiles)
            def _():
                tall_weights(after, jnp.int32(0), turn + 1).start()

    load_x = pltpu.make_async_copy(x_h, h, load_sem.at[0])
    load_dy = pltpu.make_async_copy(dy_h, dy, load_sem.at[1])
    load_x.start()
    start(wide_weights(0, jnp.int32(0)))
    tall_weights(0, jnp.int32(0), jnp.int32(0)).start()
    own_rows = pl.ds(pl.multiple_of(me * rows, 8), rows)
    first = [
        pltpu.make_async_copy(wg_h.at[0, own_rows, :], w_first, load_sem.at[2]),
        pltpu.make_async_copy(m_h.at[0], m_first, load_sem.at[3]),
        pltpu.make_async_copy(v_h.at[0], v_first, load_sem.at[4]),
    ]
    steps_away = sorted(range(1, n), key=lambda i: -min(i, n - i))
    others = [lax.rem(me + i, n) for i in steps_away]
    greet(others)
    squares[...] = jnp.zeros_like(squares)
    acc[...] = jnp.zeros_like(acc)

    def place_of(k):
        within = lax.rem(k, per_layer)
        tall = lax.div(within, 2 * tiles)
        return tall * (within - 2 * tiles + RING_GRAD) + (1 - tall) * lax.rem(within, RING_GRAD)

    def to_partner(k):
        b = lax.rem(k, RING_PARTNER)
        return pltpu.make_async_remote_copy(
            src_ref=grad.at[place_of(k), 1 - c],
            dst_ref=partner_sum.at[b],
            send_sem=d_send.at[b],
            recv_sem=d_recv.at[b],
            device_id={"dp": partner},
            device_id_type=MESH,
        )

    def target(way, s):
        return lax.rem(z + (half - s if way == 0 else chips - half + s), chips)

    def hop(way, slot, low=0, high=half - 1):
        out_b, in_b = lax.rem(slot, LAG), lax.rem(slot, slots)
        part = pl.ds(max(2 * low - 1, 0), 2 * high + 1 - max(2 * low - 1, 0))
        return pltpu.make_async_remote_copy(
            src_ref=hop_out.at[way, out_b, part],
            dst_ref=hop_in.at[way, in_b, part],
            send_sem=r_send.at[way, out_b],
            recv_sem=r_recv.at[way, in_b],
            device_id={"dp": plus if way == 0 else minus},
            device_id_type=MESH,
        )

    def first_step(k, now):
        i, b = place_of(k), lax.rem(k, RING_PARTNER)
        for way in (0, 1):
            far = target(way, 0)
            own, other = grad[i, c, far, way].astype(F32), partner_sum[b, far, way].astype(F32)
            hop_out[way, lax.rem(now, LAG), 0] = (own + other).astype(BF)

    def next_step(s, k, now):
        i, b = lax.rem(k, RING_SUM), lax.rem(now - LAG, slots)
        for way in (0, 1):
            far, to = target(way, s), hop_out.at[way, lax.rem(now, LAG)]
            for h in (0, 1):
                own = total[i, far, h]
                if s > 1:
                    own = (own.astype(F32) + hop_in[way, b, 2 * s - 3 + h].astype(F32)).astype(BF)
                elif h == way:
                    own = (own.astype(F32) + hop_in[way, b, 0].astype(F32)).astype(BF)
                to[2 * s - 1 + h] = own

    def add_partner(k):
        i, g, b = lax.rem(k, RING_SUM), place_of(k), lax.rem(k, RING_PARTNER)
        for j in range(chips):
            total[i, j] = (grad[g, c, j].astype(F32) + partner_sum[b, j].astype(F32)).astype(BF)

    def finish(k, now):
        i, b = lax.rem(k, RING_SUM), lax.rem(now - LAG, slots)
        squared = []
        for h in (0, 1):
            at_end = 2 * half - 3 + h
            g = total[i, z, h].astype(F32) + hop_in[0, b, at_end].astype(F32) + hop_in[1, b, at_end].astype(F32)
            out[k, h] = g.astype(BF)
            wide = out[k, h].astype(F32)
            squared.append(wide[0] * wide[0] + wide[1] * wide[1])
        squares[...] += squared[0] + squared[1]

    def steps(now):
        return [now - LAG_PARTNER - LAG * s for s in range(half + 1)]

    def slot(now):
        ks = steps(now)
        to_partner(now).start()
        to_partner(ks[0]).wait()
        for way in (0, 1):
            hop(way, now - LAG).wait()
        first_step(ks[0], now)
        for s in range(1, half):
            next_step(s, ks[s], now)
        finish(ks[half], now)
        for way in (0, 1):
            hop(way, now).start()
        add_partner(ks[0])

    def filling(now):
        ks = steps(now)

        @pl.when(now >= 0)
        def _():
            to_partner(now).start()

        for high in range(half):

            @pl.when((ks[high] >= LAG) & (ks[high] < 2 * LAG) if high < half - 1 else ks[high] >= LAG)
            def _(high=high):
                for way in (0, 1):
                    hop(way, now - LAG, 0, high).wait()

        @pl.when(ks[0] >= 0)
        def _():
            to_partner(ks[0]).wait()
            first_step(ks[0], now)

        for s in range(1, half):

            @pl.when(ks[s] >= 0)
            def _(s=s):
                next_step(s, ks[s], now)

        @pl.when(ks[half] >= 0)
        def _():
            finish(ks[half], now)

        for high in range(half):

            @pl.when((ks[high] >= 0) & (ks[high] < LAG) if high < half - 1 else ks[high] >= 0)
            def _(high=high):
                for way in (0, 1):
                    hop(way, now, 0, high).start()

        @pl.when(ks[0] >= 0)
        def _():
            add_partner(ks[0])

    def emptying(now):
        ks = steps(now)
        left = [k < chunks for k in ks]

        def only(low, k):
            return (k - LAG * low < chunks) & (k - LAG * low >= chunks - LAG) if low > 0 else k < chunks

        for low in range(half):

            @pl.when(only(low, ks[0] - LAG))
            def _(low=low):
                for way in (0, 1):
                    hop(way, now - LAG, low).wait()

        @pl.when(left[0])
        def _():
            to_partner(ks[0]).wait()
            first_step(ks[0], now)

        for s in range(1, half):

            @pl.when(left[s])
            def _(s=s):
                next_step(s, ks[s], now)

        finish(ks[half], now)
        for low in range(half):

            @pl.when(only(low, ks[0]))
            def _(low=low):
                for way in (0, 1):
                    hop(way, now, low).start()

        @pl.when(left[0])
        def _():
            add_partner(ks[0])

    def forward(b, a, t):
        for r in range(0, tokens, ROWS):
            mine = a[r : r + ROWS, :]
            gate = nn(mine, wg[t])
            up = nn(mine, wu[t])
            hidden = (gate * sigmoid(gate) * up).astype(BF)
            acc[r : r + ROWS, :] += nn(hidden, wd[b])

    def elementwise(b, a, t):
        for r in range(0, tokens, ROWS):
            at_rows = pl.ds(r, ROWS)
            gate = nn(a[at_rows, :], wg[t])
            up = nn(a[at_rows, :], wu[t])
            by_act = nt(dy[at_rows, :], wd[b]).astype(BF).astype(F32)
            s = sigmoid(gate)
            silu = gate * s
            act[t, at_rows, :] = (silu * up).astype(BF)
            dup[t, at_rows, :] = (by_act * silu).astype(BF)
            dgate[t, at_rows, :] = (by_act * up * (s * (1.0 + gate * (1.0 - s)))).astype(BF)

    def wide_grad(source, chunk, t):
        k = place_of(chunk)
        for p in range(2):
            g = nn(at[p * (d // 2) : (p + 1) * (d // 2), :], source[t])
            for i in range(n // 2):
                dev = p * (n // 2) + i
                for q in range(QUARTERS):
                    grad[k, dev % 2, dev // 2, q // 2, q % 2] = g[i * rows : (i + 1) * rows, q * LANES : (q + 1) * LANES].astype(BF)

    def tall_grad(t):
        per_dev = tiles * TILE // n // 8
        first_dev, first_rest = lax.div(t * (TILE // 8), per_dev), lax.rem(t * (TILE // 8), per_dev)

        def put(i, eight):
            rest = first_rest + i
            over = sum(jnp.where(rest >= per_dev * m, 1, 0) for m in range(1, TILE // 8 // per_dev + 2))
            dev, rest = first_dev + over, rest - per_dev * over
            k, quarter = RING_GRAD + (rest >> 2), rest & 3
            stacked = jnp.concatenate([eight[:, q * LANES : (q + 1) * LANES] for q in range(d // LANES)], axis=0)
            grad[k, dev & 1, dev >> 1, quarter >> 1, quarter & 1] = stacked.astype(BF)

        acc[:TILE, :] = tn(act[t], dy[...])

        def group(i, _):
            put(i, acc[pl.ds(pl.multiple_of(i * 8, 8), 8), :])
            return 0

        lax.fori_loop(0, TILE // 8, group, 0, unroll=16)

    def to_states(layer, a, first_slot):
        turn = 0
        for source, w, w_h in ((dgate, wg, wg_h), (dup, wu, wu_h)):
            for r in range(0, tokens, tokens // 2):
                at_rows = pl.ds(r, tokens // 2)
                part = nt(source[0, at_rows, :], w[0])
                for t in range(1, tiles):
                    part += nt(source[t, at_rows, :], w[t])
                if source is dgate:
                    a[at_rows, :] = part.astype(BF)
                else:
                    acc[at_rows, :] = part
                if turn < 3:
                    slot(first_slot + turn)
                    turn += 1
            which = 0 if source is dgate else 1
            for t in range(tiles):
                wide_weight(which, layer - 1, jnp.int32(t)).start()

        def norm(i, _):
            at_rows = pl.ds(pl.multiple_of(i * 32, 32), 32)
            by_a = (a[at_rows, :].astype(F32) + acc[at_rows, :].astype(BF).astype(F32)).astype(BF).astype(F32)
            wide = h[at_rows, :].astype(F32)
            scale = lax.rsqrt(jnp.mean(wide * wide, -1, keepdims=True) + 1e-6)
            along = jnp.mean(by_a * wide, -1, keepdims=True)
            by_h = (by_a * scale - wide * (scale * scale * scale * along)).astype(BF)
            dy[at_rows, :] = (dy[at_rows, :].astype(F32) + by_h.astype(F32)).astype(BF)
            return 0

        lax.fori_loop(0, tokens // 32, norm, 0, unroll=4)
        slot(first_slot + turn)

    load_x.wait()
    for t in range(1, tiles):
        start(wide_weights(0, jnp.int32(t)))
    load_dy.start()
    start(first)
    for r in range(0, tokens, 128):
        a0[r : r + 128, :] = normed(h[r : r + 128, :])

    def ahead(t):
        wait(wide_weights(0, t))
        next_tall(0, t, t, layers - 1)
        forward(lax.rem(t, 2), a0, t)
        start(wide_weights(layers - 1, t))

    each_tile(ahead)

    for r in range(0, tokens, 128):
        new = (h[r : r + 128, :].astype(F32) + acc[r : r + 128, :].astype(BF).astype(F32)).astype(BF)
        h[r : r + 128, :] = new
        a1[r : r + 128, :] = normed(new)
    at[...] = a1[...].T
    load_dy.wait()
    wait(first)
    meet(n - 1)

    for step in range(layers):
        layer = layers - 1 - step
        base = step * per_layer
        a = (a0, a1)[layer]

        def tile(t, layer=layer, base=base, a=a, step=step):
            turn = (step + 1) * tiles + t
            wait(wide_weights(layer, t))
            next_tall(layer, t, turn, layer - 1 if layer > 0 else None)
            chunk = base + 2 * t
            elementwise(lax.rem(turn, 2), a, t)
            wide_grad(dgate, chunk, t)
            if step == 0:
                filling(chunk)
                wide_grad(dup, chunk + 1, t)

                @pl.when(t + 1 < tiles)
                def _():
                    filling(chunk + 1)

            else:
                slot(chunk)
                wide_grad(dup, chunk + 1, t)
                tall_grad(t)
                slot(chunk + 1)

        each_tile(tile)
        if step == 0:

            def down(t, base=base):
                tall_grad(t)

                @pl.when(t == 1)
                def _():
                    slot(base + 2 * tiles - 1)

            each_tile(down)
            slot(base + 2 * tiles)
            to_states(layer, a, base + 2 * tiles + 1)
            at[...] = a0[...].T

    def rest(turn_of):
        def body(i, _):
            turn_of(i)
            return 0

        return body

    lax.fori_loop((layers - 1) * per_layer + 2 * tiles, chunks, rest(slot), 0)
    lax.fori_loop(chunks, chunks + full, rest(emptying), 0)

    everyone[me] = jnp.sum(squares[...].reshape(-1, 8, LANES), axis=0)

    def share(i, source):
        return pltpu.make_async_remote_copy(
            src_ref=everyone.at[source],
            dst_ref=everyone.at[source],
            send_sem=s_send.at[i],
            recv_sem=s_recv.at[i],
            device_id={"dp": others[i]},
            device_id_type=MESH,
        )

    for i in range(n - 1):
        share(i, me).start()
    for i in range(n - 1):
        share(i, lax.rem(me + n - steps_away[i], n)).wait_recv()
    square[...] = jnp.sum(everyone[...], axis=0)
    for i in range(n - 1):
        share(i, me).wait_send()


def backward(n, x, dy, wg, wu, wd, m, v):
    layers, d, ff = wg.shape
    tokens = dy.shape[0]
    tiles, rows, chips, half = ff // TILE, d // n, n // 2, n // 4
    chunks = 3 * layers * tiles
    unit = (2, 2, rows, LANES)
    hbm, vmem = pl.BlockSpec(memory_space=pl.ANY), pl.BlockSpec(memory_space=pltpu.VMEM)
    return pl.pallas_call(
        functools.partial(backward_kernel, n, layers, tiles, rows),
        in_specs=[hbm] * 7,
        out_specs=[vmem] * 5,
        out_shape=[pltpu.VMEM((chunks,) + unit, BF), pltpu.VMEM((8, LANES), F32)]
        + [pltpu.VMEM((rows, ff), dt) for dt in (BF, F32, F32)],
        scratch_shapes=[
            pltpu.VMEM((tokens, d), BF),
            pltpu.VMEM((tokens, d), BF),
            pltpu.VMEM((tokens, d), BF),
            pltpu.VMEM((d, tokens), BF),
            pltpu.VMEM((tokens, d), BF),
            pltpu.VMEM((tiles, d, TILE), BF),
            pltpu.VMEM((tiles, d, TILE), BF),
            pltpu.VMEM((2, TILE, d), BF),
            pltpu.VMEM((tiles, tokens, TILE), BF),
            pltpu.VMEM((tiles, tokens, TILE), BF),
            pltpu.VMEM((tiles, tokens, TILE), BF),
            pltpu.VMEM((tokens, d), F32),
            pltpu.VMEM((RING_GRAD + tiles, 2, chips) + unit, BF),
            pltpu.VMEM((RING_PARTNER, chips) + unit, BF),
            pltpu.VMEM((RING_SUM, chips) + unit, BF),
            pltpu.VMEM((2, LAG, 2 * half - 1) + unit[1:], BF),
            pltpu.VMEM((2, 2 * LAG, 2 * half - 1) + unit[1:], BF),
            pltpu.VMEM((rows, LANES), F32),
            pltpu.VMEM((n, 8, LANES), F32),
            pltpu.SemaphoreType.DMA((RING_PARTNER,)),
            pltpu.SemaphoreType.DMA((RING_PARTNER,)),
            pltpu.SemaphoreType.DMA((2, LAG)),
            pltpu.SemaphoreType.DMA((2, 2 * LAG)),
            pltpu.SemaphoreType.DMA((n - 1,)),
            pltpu.SemaphoreType.DMA((n - 1,)),
            pltpu.SemaphoreType.DMA((5,)),
            pltpu.SemaphoreType.DMA((2, tiles)),
            pltpu.SemaphoreType.DMA((2,)),
        ],
        compiler_params=pltpu.CompilerParams(collective_id=0, has_side_effects=True, vmem_limit_bytes=VMEM_LIMIT),
        name="backward",
    )(x, dy, wg, wu, wd, m, v)


def update_kernel(n, layers, tiles, count, *refs):
    grads, square = refs[:2]
    first = refs[2:5]
    w_h, m_h, v_h = refs[5:8], refs[8:11], refs[11:14]
    w_out, m_in, v_in = refs[14:17], refs[17:20], refs[20:23]
    w_in = refs[23:26]
    load_sem, r_send, r_recv, d_send, d_recv = refs[26:]
    chips, half = n // 2, n // 4
    me, z, c, partner, plus, minus = places(n)
    per_layer = grads.shape[0] // layers
    pieces = [(layer, i) for layer in range(layers) for i in range(3)]

    def own(ref, layer, i):
        rows = m_in[i].shape[1]
        return ref.at[layer, pl.ds(pl.multiple_of(me * rows, 8), rows), :]

    greet([partner, plus, minus])
    loads = [[]]
    for p, (layer, i) in enumerate(pieces):
        if p == 0:
            continue
        loads.append(
            [
                pltpu.make_async_copy(own(w_h[i], layer, i), w_in[i].at[layer], load_sem.at[p, 0]),
                pltpu.make_async_copy(m_h[i].at[layer], m_in[i].at[layer], load_sem.at[p, 1]),
                pltpu.make_async_copy(v_h[i].at[layer], v_in[i].at[layer], load_sem.at[p, 2]),
            ]
        )
        for one in loads[-1]:
            one.start()
    factor = jnp.minimum(1.0, 0.5 * lax.rsqrt(jnp.sum(square[...]) / count + 1e-30))

    def step(w, m, v, g):
        g = g.astype(F32) * factor
        m = 0.9 * m + 0.1 * g
        v = 0.95 * v + 0.05 * g * g
        w = w.astype(F32)
        return (w - 0.02 * (m * lax.rsqrt(v + 1e-8) + 0.1 * w)).astype(BF), m, v

    def block(ref, p, chip, core, part=None):
        layer, i = pieces[p]
        rows, cols = m_in[i].shape[1:]
        start = (chip * 2 + core) * rows
        if part is None:
            return ref.at[layer, pl.ds(pl.multiple_of(start, 8), rows), :]
        if i == 2:
            return ref.at[layer, pl.ds(pl.multiple_of(start + part * (rows // 2), 8), rows // 2), :]
        return ref.at[layer, pl.ds(pl.multiple_of(start, 8), rows), pl.ds(part * (cols // 2), cols // 2)]

    def part_of(ref, p, part):
        layer, i = pieces[p]
        rows, cols = m_in[i].shape[1:]
        if i == 2:
            return ref.at[layer, pl.ds(part * (rows // 2), rows // 2), :]
        return ref.at[layer, :, pl.ds(part * (cols // 2), cols // 2)]

    def hop(way, s, p):
        i = pieces[p][1]
        chip = lax.rem(z + (chips - s if way == 0 else s), chips)
        part = way if s == half - 1 else None
        dst = block(w_out[i], p, chip, c, part)
        if s == 0:
            src = w_in[i].at[pieces[p][0]] if part is None else part_of(w_in[i], p, part)
        else:
            src = dst
        return pltpu.make_async_remote_copy(
            src_ref=src,
            dst_ref=dst,
            send_sem=r_send.at[way, s, p],
            recv_sem=r_recv.at[way, s, p],
            device_id={"dp": plus if way == 0 else minus},
            device_id_type=MESH,
        )

    def across(j, p):
        i = pieces[p][1]
        if j == 0:
            src, dst = w_in[i].at[pieces[p][0]], block(w_out[i], p, z, c)
        else:
            s, way = (j - 1) // 2, (j - 1) % 2
            chip = lax.rem(z + (chips - 1 - s if way == 0 else 1 + s), chips)
            dst = block(w_out[i], p, chip, c, way if s == half - 1 else None)
            src = dst
        return pltpu.make_async_remote_copy(
            src_ref=src,
            dst_ref=dst,
            send_sem=d_send.at[j, p],
            recv_sem=d_recv.at[j, p],
            device_id={"dp": partner},
            device_id_type=MESH,
        )

    for p, (layer, i) in enumerate(pieces):
        for one in loads[p]:
            one.wait()
        base = (layers - 1 - layer) * per_layer
        rows, cols = m_in[i].shape[1:]
        w1, m1, v1 = w_in[i], m_in[i], v_in[i]
        if i < 2:

            def column(q, _, base=base, layer=layer, i=i, w1=w1, m1=m1, v1=v1, p=p):
                t, r = q // QUARTERS, lax.rem(q, QUARTERS)
                at_cols = pl.ds(pl.multiple_of(q * LANES, LANES), LANES)
                g = grads[base + 2 * t + i, r // 2, lax.rem(r, 2)]
                old = [one[:, at_cols] for one in first] if p == 0 else [one[layer, :, at_cols] for one in (w1, m1, v1)]
                w, m, v = step(*old, g)
                w1[layer, :, at_cols] = w
                m1[layer, :, at_cols] = m
                v1[layer, :, at_cols] = v
                return 0

            lax.fori_loop(0, cols // LANES, column, 0, unroll=5)
        else:

            def row(j, _, base=base, layer=layer, w1=w1, m1=m1, v1=v1):
                at_rows = pl.ds(pl.multiple_of(j * 32, 32), 32)
                g = grads[base + 2 * tiles + j].astype(F32)
                eights = [g[r // 2, r % 2] for r in range(4)]
                g = jnp.concatenate(
                    [jnp.concatenate([e[8 * q : 8 * q + 8, :] for q in range(cols // LANES)], axis=1) for e in eights], axis=0
                )
                w, m, v = step(w1[layer, at_rows, :], m1[layer, at_rows, :], v1[layer, at_rows, :], g)
                w1[layer, at_rows, :] = w
                m1[layer, at_rows, :] = m
                v1[layer, at_rows, :] = v
                return 0

            lax.fori_loop(0, rows // 32, row, 0, unroll=5)
        if p == 0:
            meet(3)
        for way in (0, 1):
            hop(way, 0, p).start()
        across(0, p).start()
        start = pl.ds(pl.multiple_of(me * rows, 8), rows)
        w_out[i][layer, start, :] = w1[layer]
    def settle(s, p):
        for way in (0, 1):
            hop(way, s, p).wait_send()
            across(1 + 2 * s + way, p).wait()

    for s in range(1, half + 1):
        for p in range(len(pieces)):
            if s == half:
                across(0, p).wait()
                for early in range(half - 1):
                    settle(early, p)
            for way in (0, 1):
                hop(way, s - 1, p).wait_recv()
                if s < half:
                    hop(way, s, p).start()
                across(1 + 2 * (s - 1) + way, p).start()
    for p in range(len(pieces)):
        settle(half - 1, p)


def update(n, grads, square, first, ws, ms, vs):
    layers, d, ff = ws[0].shape
    half = n // 4
    pieces = 3 * layers
    tiles = ff // TILE
    hbm, vmem = pl.BlockSpec(memory_space=pl.ANY), pl.BlockSpec(memory_space=pltpu.VMEM)
    count = sum(w.size for w in ws)
    like = lambda t, dt=None: jax.ShapeDtypeStruct(t.shape, dt or t.dtype)
    return pl.pallas_call(
        functools.partial(update_kernel, n, layers, tiles, count),
        in_specs=[vmem] * 5 + [hbm] * 9,
        out_specs=[vmem] * 9,
        out_shape=[pltpu.VMEM(t.shape, t.dtype) for t in (*ws, *ms, *vs)],
        scratch_shapes=[pltpu.VMEM(m.shape, BF) for m in ms]
        + [
            pltpu.SemaphoreType.DMA((pieces, 3)),
            pltpu.SemaphoreType.DMA((2, half, pieces)),
            pltpu.SemaphoreType.DMA((2, half, pieces)),
            pltpu.SemaphoreType.DMA((1 + 2 * half, pieces)),
            pltpu.SemaphoreType.DMA((1 + 2 * half, pieces)),
        ],
        compiler_params=pltpu.CompilerParams(collective_id=1, has_side_effects=True, vmem_limit_bytes=4_000_000),
        name="update",
    )(
        *(pltpu.with_memory_space_constraint(t, pltpu.VMEM) for t in (grads, square, *first)),
        *(pltpu.with_memory_space_constraint(t, pltpu.HBM) for t in (*ws, *ms, *vs)),
    )


def place_kernel(*refs):
    k = len(refs) // 2
    sems = refs[-1]
    layers = refs[0].shape[0]
    copies = [pltpu.make_async_copy(refs[i].at[j], refs[k + i].at[j], sems.at[i, j]) for j in range(layers) for i in range(k)]
    for one in copies:
        one.start()
    for one in copies:
        one.wait()


def place(arrays):
    hbm, vmem = pl.BlockSpec(memory_space=pl.ANY), pl.BlockSpec(memory_space=pltpu.VMEM)
    return pl.pallas_call(
        place_kernel,
        in_specs=[vmem] * len(arrays),
        out_specs=[hbm] * len(arrays),
        out_shape=[pltpu.HBM(t.shape, t.dtype) for t in arrays],
        scratch_shapes=[pltpu.SemaphoreType.DMA((len(arrays), arrays[0].shape[0]))],
        compiler_params=pltpu.CompilerParams(vmem_limit_bytes=1_000_000),
        name="place",
    )(*(pltpu.with_memory_space_constraint(t, pltpu.VMEM) for t in arrays))


def solution(mesh):
    n = mesh.shape["dp"]

    def of_a_device(x, dy, *arrays):
        ws, ms, vs = (arrays[i : i + 3] for i in (0, 3, 6))
        grads, square, *first = backward(n, x[0], dy[0], *ws, ms[0], vs[0])
        return tuple(place(update(n, grads, square, first, ws, ms, vs)))

    seq, whole, rows = P(("rep", "dp")), P(), P(None, "dp")
    return jax.shard_map(
        of_a_device,
        mesh=mesh,
        in_specs=(seq, seq) + (whole,) * 3 + (rows,) * 6,
        out_specs=(P("rep"),) * 3 + (P("rep", "dp"),) * 6,
        check_vma=False,
    )
```

```python
import functools

import jax
import jax.numpy as jnp
from jax import lax
from jax.experimental import pallas as pl
from jax.experimental.pallas import tpu as pltpu
from jax.sharding import PartitionSpec as P

MESH = pl.DeviceIdType.MESH
BF, F32 = jnp.bfloat16, jnp.float32
LANES = 128
TILE = 512
QUARTERS = TILE // LANES
ROWS = 256
LAG = 2
LAG_PARTNER = 1
RING_GRAD, RING_SUM, RING_PARTNER = 4, 10, 4
VMEM_LIMIT = 63_500_000


def nn(a, b):
    return lax.dot_general(a, b, (((1,), (0,)), ((), ())), preferred_element_type=F32)


def nt(a, b):
    return lax.dot_general(a, b, (((1,), (1,)), ((), ())), preferred_element_type=F32)


def tn(a, b):
    return lax.dot_general(a, b, (((0,), (0,)), ((), ())), preferred_element_type=F32)


def normed(h):
    wide = h.astype(F32)
    scale = lax.rsqrt(jnp.mean(wide * wide, -1, keepdims=True) + 1e-6)
    return (wide * scale).astype(BF)


def sigmoid(x):
    return 1.0 / (1.0 + jnp.exp(-x))


def places(n):
    me = lax.axis_index("dp")
    chips = n // 2
    z, c = me // 2, lax.rem(me, 2)
    plus = lax.rem(z + 1, chips) * 2 + c
    minus = lax.rem(z + chips - 1, chips) * 2 + c
    return me, z, c, z * 2 + 1 - c, plus, minus


def greet(others):
    for o in others:
        pl.semaphore_signal(pltpu.get_barrier_semaphore(), inc=1, device_id={"dp": o}, device_id_type=MESH)


def meet(count):
    pl.semaphore_wait(pltpu.get_barrier_semaphore(), count)


def backward_kernel(
    n, layers, tiles, rows,
    x_h, dy_h, wg_h, wu_h, wd_h, m_h, v_h,
    out, square, w_first, m_first, v_first,
    h, a0, a1, at, dy, wg, wu, wd, act, dgate, dup, acc,
    grad, partner_sum, total, hop_out, hop_in, squares, everyone,
    d_send, d_recv, r_send, r_recv, s_send, s_recv, x_sem, load_sem, wide_sem, tall_sem,
):
    chips, half = n // 2, n // 4
    per_layer = 3 * tiles
    chunks = layers * per_layer
    slots = 2 * LAG
    full = LAG_PARTNER + LAG * half
    me, z, c, partner, plus, minus = places(n)
    tokens, d = h.shape

    def wide_weight(i, layer, t):
        w_h, w = ((wg_h, wg), (wu_h, wu))[i]
        at_tile = pl.ds(pl.multiple_of(t * TILE, TILE), TILE)
        return pltpu.make_async_copy(w_h.at[layer, :, at_tile], w.at[t], wide_sem.at[i, t])

    def wide_weights(layer, t):
        return [wide_weight(i, layer, t) for i in (0, 1)]

    def tall_weights(layer, t, turn):
        b = lax.rem(turn, 2)
        at_tile = pl.ds(pl.multiple_of(t * TILE, TILE), TILE)
        return pltpu.make_async_copy(wd_h.at[layer, at_tile, :], wd.at[b], tall_sem.at[b])

    def each_tile(what):
        def body(t, _):
            what(t)
            return 0

        lax.fori_loop(0, tiles, body, 0)

    def start(copies):
        for one in copies:
            one.start()

    def wait(copies):
        for one in copies:
            one.wait()

    def next_tall(layer, t, turn, after):
        tall_weights(layer, t, turn).wait()

        @pl.when(t + 1 < tiles)
        def _():
            tall_weights(layer, t + 1, turn + 1).start()

        if after is not None:

            @pl.when(t + 1 == tiles)
            def _():
                tall_weights(after, jnp.int32(0), turn + 1).start()

    parts = 4
    some = tokens // parts
    load_x = [pltpu.make_async_copy(x_h.at[pl.ds(i * some, some), :], h.at[pl.ds(i * some, some), :], x_sem.at[i]) for i in range(parts)]
    load_dy = pltpu.make_async_copy(dy_h, dy, load_sem.at[1])
    start(load_x)
    steps_away = sorted(range(1, n), key=lambda i: -min(i, n - i))
    others = [lax.rem(me + i, n) for i in steps_away]
    greet(others)
    start(wide_weights(0, jnp.int32(0)))
    tall_weights(0, jnp.int32(0), jnp.int32(0)).start()
    own_rows = pl.ds(pl.multiple_of(me * rows, 8), rows)
    first = [
        pltpu.make_async_copy(wg_h.at[0, own_rows, :], w_first, load_sem.at[2]),
        pltpu.make_async_copy(m_h.at[0], m_first, load_sem.at[3]),
        pltpu.make_async_copy(v_h.at[0], v_first, load_sem.at[4]),
    ]
    squares[...] = jnp.zeros_like(squares)
    acc[...] = jnp.zeros_like(acc)

    def place_of(k):
        within = lax.rem(k, per_layer)
        tall = lax.div(within, 2 * tiles)
        return tall * (within - 2 * tiles + RING_GRAD) + (1 - tall) * lax.rem(within, RING_GRAD)

    def to_partner(k):
        b = lax.rem(k, RING_PARTNER)
        return pltpu.make_async_remote_copy(
            src_ref=grad.at[place_of(k), 1 - c],
            dst_ref=partner_sum.at[b],
            send_sem=d_send.at[b],
            recv_sem=d_recv.at[b],
            device_id={"dp": partner},
            device_id_type=MESH,
        )

    def target(way, s):
        return lax.rem(z + (half - s if way == 0 else chips - half + s), chips)

    def hop(way, slot, low=0, high=half - 1):
        out_b, in_b = lax.rem(slot, LAG), lax.rem(slot, slots)
        part = pl.ds(max(2 * low - 1, 0), 2 * high + 1 - max(2 * low - 1, 0))
        return pltpu.make_async_remote_copy(
            src_ref=hop_out.at[way, out_b, part],
            dst_ref=hop_in.at[way, in_b, part],
            send_sem=r_send.at[way, out_b],
            recv_sem=r_recv.at[way, in_b],
            device_id={"dp": plus if way == 0 else minus},
            device_id_type=MESH,
        )

    def first_step(k, now):
        i, b = place_of(k), lax.rem(k, RING_PARTNER)
        for way in (0, 1):
            far = target(way, 0)
            own, other = grad[i, c, far, way].astype(F32), partner_sum[b, far, way].astype(F32)
            hop_out[way, lax.rem(now, LAG), 0] = (own + other).astype(BF)

    def next_step(s, k, now):
        i, b = lax.rem(k, RING_SUM), lax.rem(now - LAG, slots)
        for way in (0, 1):
            far, to = target(way, s), hop_out.at[way, lax.rem(now, LAG)]
            for h in (0, 1):
                own = total[i, far, h]
                if s > 1:
                    own = (own.astype(F32) + hop_in[way, b, 2 * s - 3 + h].astype(F32)).astype(BF)
                elif h == way:
                    own = (own.astype(F32) + hop_in[way, b, 0].astype(F32)).astype(BF)
                to[2 * s - 1 + h] = own

    def add_partner(k):
        i, g, b = lax.rem(k, RING_SUM), place_of(k), lax.rem(k, RING_PARTNER)
        for j in range(chips):
            total[i, j] = (grad[g, c, j].astype(F32) + partner_sum[b, j].astype(F32)).astype(BF)

    def finish(k, now):
        i, b = lax.rem(k, RING_SUM), lax.rem(now - LAG, slots)
        squared = []
        for h in (0, 1):
            at_end = 2 * half - 3 + h
            g = total[i, z, h].astype(F32) + hop_in[0, b, at_end].astype(F32) + hop_in[1, b, at_end].astype(F32)
            out[k, h] = g.astype(BF)
            wide = out[k, h].astype(F32)
            squared.append(wide[0] * wide[0] + wide[1] * wide[1])
        squares[...] += squared[0] + squared[1]

    def steps(now):
        return [now - LAG_PARTNER - LAG * s for s in range(half + 1)]

    def slot(now):
        ks = steps(now)
        to_partner(now).start()
        to_partner(ks[0]).wait()
        for way in (0, 1):
            hop(way, now - LAG).wait()
        first_step(ks[0], now)
        for s in range(1, half):
            next_step(s, ks[s], now)
        finish(ks[half], now)
        for way in (0, 1):
            hop(way, now).start()
        add_partner(ks[0])

    def filling(now):
        ks = steps(now)

        @pl.when(now >= 0)
        def _():
            to_partner(now).start()

        for high in range(half):

            @pl.when((ks[high] >= LAG) & (ks[high] < 2 * LAG) if high < half - 1 else ks[high] >= LAG)
            def _(high=high):
                for way in (0, 1):
                    hop(way, now - LAG, 0, high).wait()

        @pl.when(ks[0] >= 0)
        def _():
            to_partner(ks[0]).wait()
            first_step(ks[0], now)

        for s in range(1, half):

            @pl.when(ks[s] >= 0)
            def _(s=s):
                next_step(s, ks[s], now)

        @pl.when(ks[half] >= 0)
        def _():
            finish(ks[half], now)

        for high in range(half):

            @pl.when((ks[high] >= 0) & (ks[high] < LAG) if high < half - 1 else ks[high] >= 0)
            def _(high=high):
                for way in (0, 1):
                    hop(way, now, 0, high).start()

        @pl.when(ks[0] >= 0)
        def _():
            add_partner(ks[0])

    def emptying(now):
        ks = steps(now)
        left = [k < chunks for k in ks]

        def only(low, k):
            return (k - LAG * low < chunks) & (k - LAG * low >= chunks - LAG) if low > 0 else k < chunks

        for low in range(half):

            @pl.when(only(low, ks[0] - LAG))
            def _(low=low):
                for way in (0, 1):
                    hop(way, now - LAG, low).wait()

        @pl.when(left[0])
        def _():
            to_partner(ks[0]).wait()
            first_step(ks[0], now)

        for s in range(1, half):

            @pl.when(left[s])
            def _(s=s):
                next_step(s, ks[s], now)

        finish(ks[half], now)
        for low in range(half):

            @pl.when(only(low, ks[0]))
            def _(low=low):
                for way in (0, 1):
                    hop(way, now, low).start()

        @pl.when(left[0])
        def _():
            add_partner(ks[0])

    def forward(b, a, t):
        def hidden(r):
            mine = a[r : r + ROWS, :]
            gate = nn(mine, wg[t])
            up = nn(mine, wu[t])
            return (gate * sigmoid(gate) * up).astype(BF)

        ready = hidden(0)
        for r in range(0, tokens, ROWS):
            following = hidden(r + ROWS) if r + ROWS < tokens else None
            acc[r : r + ROWS, :] += nn(ready, wd[b])
            ready = following

    def elementwise(b, a, t):
        for r in range(0, tokens, ROWS):
            at_rows = pl.ds(r, ROWS)
            gate = nn(a[at_rows, :], wg[t])
            up = nn(a[at_rows, :], wu[t])
            by_act = nt(dy[at_rows, :], wd[b]).astype(BF).astype(F32)
            s = sigmoid(gate)
            silu = gate * s
            act[t, at_rows, :] = (silu * up).astype(BF)
            dup[t, at_rows, :] = (by_act * silu).astype(BF)
            dgate[t, at_rows, :] = (by_act * up * (s * (1.0 + gate * (1.0 - s)))).astype(BF)

    def wide_grad(source, chunk, t):
        k = place_of(chunk)
        for p in range(2):
            g = nn(at[p * (d // 2) : (p + 1) * (d // 2), :], source[t])
            for i in range(n // 2):
                dev = p * (n // 2) + i
                for q in range(QUARTERS):
                    grad[k, dev % 2, dev // 2, q // 2, q % 2] = g[i * rows : (i + 1) * rows, q * LANES : (q + 1) * LANES].astype(BF)

    def tall_grad(t):
        acc[pl.ds(pl.multiple_of(lax.rem(t, 2) * TILE, TILE), TILE), :] = tn(act[t], dy[...])

    def tall_place(t):
        per_dev = tiles * TILE // n // 16
        first_dev, first_rest = lax.div(t * (TILE // 16), per_dev), lax.rem(t * (TILE // 16), per_dev)
        offset = lax.rem(t, 2) * TILE
        for i in range(TILE // 16):
            rest = first_rest + i
            low, high = i // per_dev, (i + per_dev - 1) // per_dev
            over = low if low == high else low + jnp.where(rest >= per_dev * high, 1, 0)
            dev, rest = first_dev + over, rest - per_dev * over
            to = grad.at[RING_GRAD + (rest >> 1), dev & 1, dev >> 1, rest & 1]
            for e in (0, 1):
                eight = acc[pl.ds(pl.multiple_of(offset + 16 * i + 8 * e, 8), 8), :]
                stacked = jnp.concatenate([eight[:, q * LANES : (q + 1) * LANES] for q in range(d // LANES)], axis=0)
                to[e] = stacked.astype(BF)

    def tall_turn(t):
        tall_place(lax.rem(t + tiles - 1, tiles))
        tall_grad(t)

    def to_states(layer, a, first_slot):
        turn = 0
        for source, w, w_h in ((dgate, wg, wg_h), (dup, wu, wu_h)):
            for r in range(0, tokens, tokens // 2):
                at_rows = pl.ds(r, tokens // 2)
                part = nt(source[0, at_rows, :], w[0])
                for t in range(1, tiles):
                    part += nt(source[t, at_rows, :], w[t])
                if source is dgate:
                    a[at_rows, :] = part.astype(BF)
                else:
                    acc[at_rows, :] = part
                if turn < 3:
                    slot(first_slot + turn)
                    turn += 1
            which = 0 if source is dgate else 1
            for t in range(tiles):
                wide_weight(which, layer - 1, jnp.int32(t)).start()

        for r in range(0, tokens, 128):
            at_rows = pl.ds(r, 128)
            by_a = (a[at_rows, :].astype(F32) + acc[at_rows, :].astype(BF).astype(F32)).astype(BF).astype(F32)
            wide = h[at_rows, :].astype(F32)
            scale = lax.rsqrt(jnp.mean(wide * wide, -1, keepdims=True) + 1e-6)
            along = jnp.mean(by_a * wide, -1, keepdims=True)
            by_h = (by_a * scale - wide * (scale * scale * scale * along)).astype(BF)
            dy[at_rows, :] = (dy[at_rows, :].astype(F32) + by_h.astype(F32)).astype(BF)
        slot(first_slot + turn)

    for i in range(parts):
        load_x[i].wait()
        if i == parts - 1:
            for t in range(1, tiles):
                start(wide_weights(0, jnp.int32(t)))
            load_dy.start()
            start(first)
        for r in range(i * some, (i + 1) * some, 128):
            a0[r : r + 128, :] = normed(h[r : r + 128, :])

    def ahead(t):
        wait(wide_weights(0, t))
        next_tall(0, t, t, layers - 1)
        forward(lax.rem(t, 2), a0, t)
        start(wide_weights(layers - 1, t))

    each_tile(ahead)

    for r in range(0, tokens, 128):
        new = (h[r : r + 128, :].astype(F32) + acc[r : r + 128, :].astype(BF).astype(F32)).astype(BF)
        h[r : r + 128, :] = new
        new = normed(new)
        a1[r : r + 128, :] = new
        at[:, r : r + 128] = new.T
    load_dy.wait()
    wait(first)
    meet(n - 1)

    for step in range(layers):
        layer = layers - 1 - step
        base = step * per_layer
        a = (a0, a1)[layer]

        def tile(t, layer=layer, base=base, a=a, step=step):
            turn = (step + 1) * tiles + t
            wait(wide_weights(layer, t))
            next_tall(layer, t, turn, layer - 1 if layer > 0 else None)
            chunk = base + 2 * t
            elementwise(lax.rem(turn, 2), a, t)
            wide_grad(dgate, chunk, t)
            if step == 0:
                filling(chunk)
                wide_grad(dup, chunk + 1, t)

                @pl.when(t + 1 < tiles)
                def _():
                    filling(chunk + 1)

            else:
                slot(chunk)
                tall_place(lax.rem(t + tiles - 1, tiles))
                wide_grad(dup, chunk + 1, t)
                tall_grad(t)
                slot(chunk + 1)

        each_tile(tile)
        if step > 0:
            tall_place(jnp.int32(tiles - 1))
        if step == 0:

            def down(t, base=base):
                tall_turn(t)

                @pl.when(t == 1)
                def _():
                    slot(base + 2 * tiles - 1)

            each_tile(down)
            tall_place(jnp.int32(tiles - 1))
            slot(base + 2 * tiles)
            to_states(layer, a, base + 2 * tiles + 1)
            at[...] = a0[...].T

    def rest(turn_of):
        def body(i, _):
            turn_of(i)
            return 0

        return body

    lax.fori_loop((layers - 1) * per_layer + 2 * tiles, chunks, rest(slot), 0)
    lax.fori_loop(chunks, chunks + full, rest(emptying), 0)

    everyone[me] = jnp.sum(squares[...].reshape(-1, 8, LANES), axis=0)

    def share(i, source):
        return pltpu.make_async_remote_copy(
            src_ref=everyone.at[source],
            dst_ref=everyone.at[source],
            send_sem=s_send.at[i],
            recv_sem=s_recv.at[i],
            device_id={"dp": others[i]},
            device_id_type=MESH,
        )

    for i in range(n - 1):
        share(i, me).start()
    for i in range(n - 1):
        share(i, lax.rem(me + n - steps_away[i], n)).wait_recv()
    square[...] = jnp.sum(everyone[...], axis=0)
    for i in range(n - 1):
        share(i, me).wait_send()


def backward(n, x, dy, wg, wu, wd, m, v):
    layers, d, ff = wg.shape
    tokens = dy.shape[0]
    tiles, rows, chips, half = ff // TILE, d // n, n // 2, n // 4
    chunks = 3 * layers * tiles
    unit = (2, 2, rows, LANES)
    hbm, vmem = pl.BlockSpec(memory_space=pl.ANY), pl.BlockSpec(memory_space=pltpu.VMEM)
    return pl.pallas_call(
        functools.partial(backward_kernel, n, layers, tiles, rows),
        in_specs=[hbm] * 7,
        out_specs=[vmem] * 5,
        out_shape=[pltpu.VMEM((chunks,) + unit, BF), pltpu.VMEM((8, LANES), F32)]
        + [pltpu.VMEM((rows, ff), dt) for dt in (BF, F32, F32)],
        scratch_shapes=[
            pltpu.VMEM((tokens, d), BF),
            pltpu.VMEM((tokens, d), BF),
            pltpu.VMEM((tokens, d), BF),
            pltpu.VMEM((d, tokens), BF),
            pltpu.VMEM((tokens, d), BF),
            pltpu.VMEM((tiles, d, TILE), BF),
            pltpu.VMEM((tiles, d, TILE), BF),
            pltpu.VMEM((2, TILE, d), BF),
            pltpu.VMEM((tiles, tokens, TILE), BF),
            pltpu.VMEM((tiles, tokens, TILE), BF),
            pltpu.VMEM((tiles, tokens, TILE), BF),
            pltpu.VMEM((tokens, d), F32),
            pltpu.VMEM((RING_GRAD + tiles, 2, chips) + unit, BF),
            pltpu.VMEM((RING_PARTNER, chips) + unit, BF),
            pltpu.VMEM((RING_SUM, chips) + unit, BF),
            pltpu.VMEM((2, LAG, 2 * half - 1) + unit[1:], BF),
            pltpu.VMEM((2, 2 * LAG, 2 * half - 1) + unit[1:], BF),
            pltpu.VMEM((rows, LANES), F32),
            pltpu.VMEM((n, 8, LANES), F32),
            pltpu.SemaphoreType.DMA((RING_PARTNER,)),
            pltpu.SemaphoreType.DMA((RING_PARTNER,)),
            pltpu.SemaphoreType.DMA((2, LAG)),
            pltpu.SemaphoreType.DMA((2, 2 * LAG)),
            pltpu.SemaphoreType.DMA((n - 1,)),
            pltpu.SemaphoreType.DMA((n - 1,)),
            pltpu.SemaphoreType.DMA((4,)),
            pltpu.SemaphoreType.DMA((5,)),
            pltpu.SemaphoreType.DMA((2, tiles)),
            pltpu.SemaphoreType.DMA((2,)),
        ],
        compiler_params=pltpu.CompilerParams(collective_id=0, has_side_effects=True, vmem_limit_bytes=VMEM_LIMIT),
        name="backward",
    )(x, dy, wg, wu, wd, m, v)


def update_kernel(n, layers, tiles, count, *refs):
    grads, square = refs[:2]
    first = refs[2:5]
    w_h, m_h, v_h = refs[5:8], refs[8:11], refs[11:14]
    w_out, m_in, v_in = refs[14:17], refs[17:20], refs[20:23]
    w_in = refs[23:26]
    load_sem, r_send, r_recv, d_send, d_recv = refs[26:]
    chips, half = n // 2, n // 4
    me, z, c, partner, plus, minus = places(n)
    per_layer = grads.shape[0] // layers
    pieces = [(layer, i) for layer in range(layers) for i in range(3)]

    def own(ref, layer, i):
        rows = m_in[i].shape[1]
        return ref.at[layer, pl.ds(pl.multiple_of(me * rows, 8), rows), :]

    greet([partner, plus, minus])
    loads = [[]]
    for p, (layer, i) in enumerate(pieces):
        if p == 0:
            continue
        loads.append(
            [
                pltpu.make_async_copy(own(w_h[i], layer, i), w_in[i].at[layer], load_sem.at[p, 0]),
                pltpu.make_async_copy(m_h[i].at[layer], m_in[i].at[layer], load_sem.at[p, 1]),
                pltpu.make_async_copy(v_h[i].at[layer], v_in[i].at[layer], load_sem.at[p, 2]),
            ]
        )
        for one in loads[-1]:
            one.start()
    factor = jnp.minimum(1.0, 0.5 * lax.rsqrt(jnp.sum(square[...]) / count + 1e-30))

    def step(w, m, v, g):
        g = g.astype(F32) * factor
        m = 0.9 * m + 0.1 * g
        v = 0.95 * v + 0.05 * g * g
        w = w.astype(F32)
        return (w - 0.02 * (m * lax.rsqrt(v + 1e-8) + 0.1 * w)).astype(BF), m, v

    def block(ref, p, chip, core, part=None):
        layer, i = pieces[p]
        rows, cols = m_in[i].shape[1:]
        start = (chip * 2 + core) * rows
        if part is None:
            return ref.at[layer, pl.ds(pl.multiple_of(start, 8), rows), :]
        if i == 2:
            return ref.at[layer, pl.ds(pl.multiple_of(start + part * (rows // 2), 8), rows // 2), :]
        return ref.at[layer, pl.ds(pl.multiple_of(start, 8), rows), pl.ds(part * (cols // 2), cols // 2)]

    def part_of(ref, p, part):
        layer, i = pieces[p]
        rows, cols = m_in[i].shape[1:]
        if i == 2:
            return ref.at[layer, pl.ds(part * (rows // 2), rows // 2), :]
        return ref.at[layer, :, pl.ds(part * (cols // 2), cols // 2)]

    def hop(way, s, p):
        i = pieces[p][1]
        chip = lax.rem(z + (chips - s if way == 0 else s), chips)
        part = way if s == half - 1 else None
        dst = block(w_out[i], p, chip, c, part)
        if s == 0:
            src = w_in[i].at[pieces[p][0]] if part is None else part_of(w_in[i], p, part)
        else:
            src = dst
        return pltpu.make_async_remote_copy(
            src_ref=src,
            dst_ref=dst,
            send_sem=r_send.at[way, s, p],
            recv_sem=r_recv.at[way, s, p],
            device_id={"dp": plus if way == 0 else minus},
            device_id_type=MESH,
        )

    def across(j, p):
        i = pieces[p][1]
        if j == 0:
            src, dst = w_in[i].at[pieces[p][0]], block(w_out[i], p, z, c)
        else:
            s, way = (j - 1) // 2, (j - 1) % 2
            chip = lax.rem(z + (chips - 1 - s if way == 0 else 1 + s), chips)
            dst = block(w_out[i], p, chip, c, way if s == half - 1 else None)
            src = dst
        return pltpu.make_async_remote_copy(
            src_ref=src,
            dst_ref=dst,
            send_sem=d_send.at[j, p],
            recv_sem=d_recv.at[j, p],
            device_id={"dp": partner},
            device_id_type=MESH,
        )

    for p, (layer, i) in enumerate(pieces):
        for one in loads[p]:
            one.wait()
        base = (layers - 1 - layer) * per_layer
        rows, cols = m_in[i].shape[1:]
        w1, m1, v1 = w_in[i], m_in[i], v_in[i]
        if i < 2:

            def column(q, _, base=base, layer=layer, i=i, w1=w1, m1=m1, v1=v1, p=p):
                t, r = q // QUARTERS, lax.rem(q, QUARTERS)
                at_cols = pl.ds(pl.multiple_of(q * LANES, LANES), LANES)
                g = grads[base + 2 * t + i, r // 2, lax.rem(r, 2)]
                old = [one[:, at_cols] for one in first] if p == 0 else [one[layer, :, at_cols] for one in (w1, m1, v1)]
                w, m, v = step(*old, g)
                w1[layer, :, at_cols] = w
                m1[layer, :, at_cols] = m
                v1[layer, :, at_cols] = v
                return 0

            lax.fori_loop(0, cols // LANES, column, 0, unroll=5)
        else:

            def row(j, _, base=base, layer=layer, w1=w1, m1=m1, v1=v1):
                at_rows = pl.ds(pl.multiple_of(j * 32, 32), 32)
                g = grads[base + 2 * tiles + j].astype(F32)
                eights = [g[r // 2, r % 2] for r in range(4)]
                g = jnp.concatenate(
                    [jnp.concatenate([e[8 * q : 8 * q + 8, :] for q in range(cols // LANES)], axis=1) for e in eights], axis=0
                )
                w, m, v = step(w1[layer, at_rows, :], m1[layer, at_rows, :], v1[layer, at_rows, :], g)
                w1[layer, at_rows, :] = w
                m1[layer, at_rows, :] = m
                v1[layer, at_rows, :] = v
                return 0

            lax.fori_loop(0, rows // 32, row, 0, unroll=5)
        if p == 0:
            meet(3)
        for way in (0, 1):
            hop(way, 0, p).start()
        across(0, p).start()
        start = pl.ds(pl.multiple_of(me * rows, 8), rows)
        w_out[i][layer, start, :] = w1[layer]
    def settle(s, p):
        for way in (0, 1):
            hop(way, s, p).wait_send()
            across(1 + 2 * s + way, p).wait()

    for s in range(1, half + 1):
        for p in range(len(pieces)):
            if s == half:
                across(0, p).wait()
                for early in range(half - 1):
                    settle(early, p)
            for way in (0, 1):
                hop(way, s - 1, p).wait_recv()
                if s < half:
                    hop(way, s, p).start()
                across(1 + 2 * (s - 1) + way, p).start()
    for p in range(len(pieces)):
        settle(half - 1, p)


def update(n, grads, square, first, ws, ms, vs):
    layers, d, ff = ws[0].shape
    half = n // 4
    pieces = 3 * layers
    tiles = ff // TILE
    hbm, vmem = pl.BlockSpec(memory_space=pl.ANY), pl.BlockSpec(memory_space=pltpu.VMEM)
    count = sum(w.size for w in ws)
    like = lambda t, dt=None: jax.ShapeDtypeStruct(t.shape, dt or t.dtype)
    return pl.pallas_call(
        functools.partial(update_kernel, n, layers, tiles, count),
        in_specs=[vmem] * 5 + [hbm] * 9,
        out_specs=[vmem] * 9,
        out_shape=[pltpu.VMEM(t.shape, t.dtype) for t in (*ws, *ms, *vs)],
        scratch_shapes=[pltpu.VMEM(m.shape, BF) for m in ms]
        + [
            pltpu.SemaphoreType.DMA((pieces, 3)),
            pltpu.SemaphoreType.DMA((2, half, pieces)),
            pltpu.SemaphoreType.DMA((2, half, pieces)),
            pltpu.SemaphoreType.DMA((1 + 2 * half, pieces)),
            pltpu.SemaphoreType.DMA((1 + 2 * half, pieces)),
        ],
        compiler_params=pltpu.CompilerParams(collective_id=1, has_side_effects=True, vmem_limit_bytes=4_000_000),
        name="update",
    )(
        *(pltpu.with_memory_space_constraint(t, pltpu.VMEM) for t in (grads, square, *first)),
        *(pltpu.with_memory_space_constraint(t, pltpu.HBM) for t in (*ws, *ms, *vs)),
    )


def place_kernel(*refs):
    k = len(refs) // 2
    sems = refs[-1]
    layers = refs[0].shape[0]
    copies = [pltpu.make_async_copy(refs[i].at[j], refs[k + i].at[j], sems.at[i, j]) for j in range(layers) for i in range(k)]
    for one in copies:
        one.start()
    for one in copies:
        one.wait()


def place(arrays):
    hbm, vmem = pl.BlockSpec(memory_space=pl.ANY), pl.BlockSpec(memory_space=pltpu.VMEM)
    return pl.pallas_call(
        place_kernel,
        in_specs=[vmem] * len(arrays),
        out_specs=[hbm] * len(arrays),
        out_shape=[pltpu.HBM(t.shape, t.dtype) for t in arrays],
        scratch_shapes=[pltpu.SemaphoreType.DMA((len(arrays), arrays[0].shape[0]))],
        compiler_params=pltpu.CompilerParams(vmem_limit_bytes=1_000_000),
        name="place",
    )(*(pltpu.with_memory_space_constraint(t, pltpu.VMEM) for t in arrays))


def solution(mesh):
    n = mesh.shape["dp"]

    def of_a_device(x, dy, *arrays):
        ws, ms, vs = (arrays[i : i + 3] for i in (0, 3, 6))
        grads, square, *first = backward(n, x[0], dy[0], *ws, ms[0], vs[0])
        return tuple(place(update(n, grads, square, first, ws, ms, vs)))

    seq, whole, rows = P(("rep", "dp")), P(), P(None, "dp")
    return jax.shard_map(
        of_a_device,
        mesh=mesh,
        in_specs=(seq, seq) + (whole,) * 3 + (rows,) * 6,
        out_specs=(P("rep"),) * 3 + (P("rep", "dp"),) * 6,
        check_vma=False,
    )
```

```python
import functools

import jax
import jax.numpy as jnp
from jax import lax
from jax.experimental import pallas as pl
from jax.experimental.pallas import tpu as pltpu
from jax.sharding import PartitionSpec as P

MESH = pl.DeviceIdType.MESH
BF, F32 = jnp.bfloat16, jnp.float32
LANES = 128
TILE = 512
QUARTERS = TILE // LANES
ROWS = 256
LAG = 2
LAG_PARTNER = 1
RING_GRAD, RING_SUM, RING_PARTNER = 4, 10, 4
VMEM_LIMIT = 63_500_000


def nn(a, b):
    return lax.dot_general(a, b, (((1,), (0,)), ((), ())), preferred_element_type=F32)


def nt(a, b):
    return lax.dot_general(a, b, (((1,), (1,)), ((), ())), preferred_element_type=F32)


def tn(a, b):
    return lax.dot_general(a, b, (((0,), (0,)), ((), ())), preferred_element_type=F32)


def normed(h):
    wide = h.astype(F32)
    scale = lax.rsqrt(jnp.mean(wide * wide, -1, keepdims=True) + 1e-6)
    return (wide * scale).astype(BF)


def sigmoid(x):
    return 1.0 / (1.0 + jnp.exp(-x))


def places(n):
    me = lax.axis_index("dp")
    chips = n // 2
    z, c = me // 2, lax.rem(me, 2)
    plus = lax.rem(z + 1, chips) * 2 + c
    minus = lax.rem(z + chips - 1, chips) * 2 + c
    return me, z, c, z * 2 + 1 - c, plus, minus


def greet(others):
    for o in others:
        pl.semaphore_signal(pltpu.get_barrier_semaphore(), inc=1, device_id={"dp": o}, device_id_type=MESH)


def meet(count):
    pl.semaphore_wait(pltpu.get_barrier_semaphore(), count)


def backward_kernel(
    n, layers, tiles, rows,
    x_h, dy_h, wg_h, wu_h, wd_h, m_h, v_h,
    out, square, w_first, m_first, v_first,
    h, a0, a1, at, dy, wg, wu, wd, act, dgate, dup, acc,
    grad, partner_sum, total, hop_out, hop_in, squares, everyone,
    d_send, d_recv, r_send, r_recv, s_send, s_recv, x_sem, load_sem, wide_sem, tall_sem,
):
    chips, half = n // 2, n // 4
    per_layer = 3 * tiles
    chunks = layers * per_layer
    slots = 2 * LAG
    full = LAG_PARTNER + LAG * half
    me, z, c, partner, plus, minus = places(n)
    tokens, d = h.shape

    def wide_weight(i, layer, t):
        w_h, w = ((wg_h, wg), (wu_h, wu))[i]
        at_tile = pl.ds(pl.multiple_of(t * TILE, TILE), TILE)
        return pltpu.make_async_copy(w_h.at[layer, :, at_tile], w.at[t], wide_sem.at[i, t])

    def wide_weights(layer, t):
        return [wide_weight(i, layer, t) for i in (0, 1)]

    def tall_weights(layer, t, turn):
        b = lax.rem(turn, 2)
        at_tile = pl.ds(pl.multiple_of(t * TILE, TILE), TILE)
        return pltpu.make_async_copy(wd_h.at[layer, at_tile, :], wd.at[b], tall_sem.at[b])

    def each_tile(what):
        def body(t, _):
            what(t)
            return 0

        lax.fori_loop(0, tiles, body, 0)

    def start(copies):
        for one in copies:
            one.start()

    def wait(copies):
        for one in copies:
            one.wait()

    def next_tall(layer, t, turn, after):
        tall_weights(layer, t, turn).wait()

        @pl.when(t + 1 < tiles)
        def _():
            tall_weights(layer, t + 1, turn + 1).start()

        if after is not None:

            @pl.when(t + 1 == tiles)
            def _():
                tall_weights(after, jnp.int32(0), turn + 1).start()

    parts = 4
    some = tokens // parts
    load_x = [pltpu.make_async_copy(x_h.at[pl.ds(i * some, some), :], h.at[pl.ds(i * some, some), :], x_sem.at[i]) for i in range(parts)]
    load_dy = pltpu.make_async_copy(dy_h, dy, load_sem.at[1])
    start(load_x)
    steps_away = sorted(range(1, n), key=lambda i: -min(i, n - i))
    others = [lax.rem(me + i, n) for i in steps_away]
    greet(others)
    start(wide_weights(0, jnp.int32(0)))
    tall_weights(0, jnp.int32(0), jnp.int32(0)).start()
    own_rows = pl.ds(pl.multiple_of(me * rows, 8), rows)
    first = [
        pltpu.make_async_copy(wg_h.at[0, own_rows, :], w_first, load_sem.at[2]),
        pltpu.make_async_copy(m_h.at[0], m_first, load_sem.at[3]),
        pltpu.make_async_copy(v_h.at[0], v_first, load_sem.at[4]),
    ]
    squares[...] = jnp.zeros_like(squares)
    acc[...] = jnp.zeros_like(acc)

    def place_of(k):
        within = lax.rem(k, per_layer)
        tall = lax.div(within, 2 * tiles)
        return tall * (within - 2 * tiles + RING_GRAD) + (1 - tall) * lax.rem(within, RING_GRAD)

    def to_partner(k):
        b = lax.rem(k, RING_PARTNER)
        return pltpu.make_async_remote_copy(
            src_ref=grad.at[place_of(k), 1 - c],
            dst_ref=partner_sum.at[b],
            send_sem=d_send.at[b],
            recv_sem=d_recv.at[b],
            device_id={"dp": partner},
            device_id_type=MESH,
        )

    def target(way, s):
        return lax.rem(z + (half - s if way == 0 else chips - half + s), chips)

    def hop(way, slot, low=0, high=half - 1):
        out_b, in_b = lax.rem(slot, LAG), lax.rem(slot, slots)
        part = pl.ds(max(2 * low - 1, 0), 2 * high + 1 - max(2 * low - 1, 0))
        return pltpu.make_async_remote_copy(
            src_ref=hop_out.at[way, out_b, part],
            dst_ref=hop_in.at[way, in_b, part],
            send_sem=r_send.at[way, out_b],
            recv_sem=r_recv.at[way, in_b],
            device_id={"dp": plus if way == 0 else minus},
            device_id_type=MESH,
        )

    def first_step(k, now):
        i, b = place_of(k), lax.rem(k, RING_PARTNER)
        for way in (0, 1):
            far = target(way, 0)
            own, other = grad[i, c, far, way].astype(F32), partner_sum[b, far, way].astype(F32)
            hop_out[way, lax.rem(now, LAG), 0] = (own + other).astype(BF)

    def next_step(s, k, now):
        i, b = lax.rem(k, RING_SUM), lax.rem(now - LAG, slots)
        for way in (0, 1):
            far, to = target(way, s), hop_out.at[way, lax.rem(now, LAG)]
            for h in (0, 1):
                own = total[i, far, h]
                if s > 1:
                    own = (own.astype(F32) + hop_in[way, b, 2 * s - 3 + h].astype(F32)).astype(BF)
                elif h == way:
                    own = (own.astype(F32) + hop_in[way, b, 0].astype(F32)).astype(BF)
                to[2 * s - 1 + h] = own

    def add_partner(k):
        i, g, b = lax.rem(k, RING_SUM), place_of(k), lax.rem(k, RING_PARTNER)
        for j in range(chips):
            total[i, j] = (grad[g, c, j].astype(F32) + partner_sum[b, j].astype(F32)).astype(BF)

    def finish(k, now):
        i, b = lax.rem(k, RING_SUM), lax.rem(now - LAG, slots)
        squared = []
        for h in (0, 1):
            at_end = 2 * half - 3 + h
            g = total[i, z, h].astype(F32) + hop_in[0, b, at_end].astype(F32) + hop_in[1, b, at_end].astype(F32)
            out[k, h] = g.astype(BF)
            wide = out[k, h].astype(F32)
            squared.append(wide[0] * wide[0] + wide[1] * wide[1])
        squares[...] += squared[0] + squared[1]

    def steps(now):
        return [now - LAG_PARTNER - LAG * s for s in range(half + 1)]

    def slot(now):
        ks = steps(now)
        to_partner(now).start()
        to_partner(ks[0]).wait()
        for way in (0, 1):
            hop(way, now - LAG).wait()
        first_step(ks[0], now)
        for s in range(1, half):
            next_step(s, ks[s], now)
        finish(ks[half], now)
        for way in (0, 1):
            hop(way, now).start()
        add_partner(ks[0])

    def filling(now):
        ks = steps(now)

        @pl.when(now >= 0)
        def _():
            to_partner(now).start()

        for high in range(half):

            @pl.when((ks[high] >= LAG) & (ks[high] < 2 * LAG) if high < half - 1 else ks[high] >= LAG)
            def _(high=high):
                for way in (0, 1):
                    hop(way, now - LAG, 0, high).wait()

        @pl.when(ks[0] >= 0)
        def _():
            to_partner(ks[0]).wait()
            first_step(ks[0], now)

        for s in range(1, half):

            @pl.when(ks[s] >= 0)
            def _(s=s):
                next_step(s, ks[s], now)

        @pl.when(ks[half] >= 0)
        def _():
            finish(ks[half], now)

        for high in range(half):

            @pl.when((ks[high] >= 0) & (ks[high] < LAG) if high < half - 1 else ks[high] >= 0)
            def _(high=high):
                for way in (0, 1):
                    hop(way, now, 0, high).start()

        @pl.when(ks[0] >= 0)
        def _():
            add_partner(ks[0])

    def emptying(now):
        ks = steps(now)
        left = [k < chunks for k in ks]

        def only(low, k):
            return (k - LAG * low < chunks) & (k - LAG * low >= chunks - LAG) if low > 0 else k < chunks

        for low in range(half):

            @pl.when(only(low, ks[0] - LAG))
            def _(low=low):
                for way in (0, 1):
                    hop(way, now - LAG, low).wait()

        @pl.when(left[0])
        def _():
            to_partner(ks[0]).wait()
            first_step(ks[0], now)

        for s in range(1, half):

            @pl.when(left[s])
            def _(s=s):
                next_step(s, ks[s], now)

        finish(ks[half], now)
        for low in range(half):

            @pl.when(only(low, ks[0]))
            def _(low=low):
                for way in (0, 1):
                    hop(way, now, low).start()

        @pl.when(left[0])
        def _():
            add_partner(ks[0])

    def forward(b, a, t):
        def hidden(r):
            mine = a[r : r + ROWS, :]
            gate = nn(mine, wg[t])
            up = nn(mine, wu[t])
            return (gate * sigmoid(gate) * up).astype(BF)

        ready = hidden(0)
        for r in range(0, tokens, ROWS):
            following = hidden(r + ROWS) if r + ROWS < tokens else None
            acc[r : r + ROWS, :] += nn(ready, wd[b])
            ready = following

    def elementwise(b, a, t):
        for r in range(0, tokens, ROWS):
            at_rows = pl.ds(r, ROWS)
            gate = nn(a[at_rows, :], wg[t])
            up = nn(a[at_rows, :], wu[t])
            by_act = nt(dy[at_rows, :], wd[b]).astype(BF).astype(F32)
            s = sigmoid(gate)
            silu = gate * s
            act[t, at_rows, :] = (silu * up).astype(BF)
            dup[t, at_rows, :] = (by_act * silu).astype(BF)
            dgate[t, at_rows, :] = (by_act * up * (s * (1.0 + gate * (1.0 - s)))).astype(BF)

    def wide_grad(source, chunk, t):
        k = place_of(chunk)
        for p in range(2):
            g = nn(at[p * (d // 2) : (p + 1) * (d // 2), :], source[t])
            for i in range(n // 2):
                dev = p * (n // 2) + i
                for q in range(QUARTERS):
                    grad[k, dev % 2, dev // 2, q // 2, q % 2] = g[i * rows : (i + 1) * rows, q * LANES : (q + 1) * LANES].astype(BF)

    def tall_grad(t):
        acc[pl.ds(pl.multiple_of(lax.rem(t, 2) * TILE, TILE), TILE), :] = tn(act[t], dy[...])

    def tall_place(t):
        per_dev = tiles * TILE // n // 16
        first_dev, first_rest = lax.div(t * (TILE // 16), per_dev), lax.rem(t * (TILE // 16), per_dev)
        offset = lax.rem(t, 2) * TILE
        for i in range(TILE // 16):
            rest = first_rest + i
            low, high = i // per_dev, (i + per_dev - 1) // per_dev
            over = low if low == high else low + jnp.where(rest >= per_dev * high, 1, 0)
            dev, rest = first_dev + over, rest - per_dev * over
            to = grad.at[RING_GRAD + (rest >> 1), dev & 1, dev >> 1, rest & 1]
            for e in (0, 1):
                eight = acc[pl.ds(pl.multiple_of(offset + 16 * i + 8 * e, 8), 8), :]
                stacked = jnp.concatenate([eight[:, q * LANES : (q + 1) * LANES] for q in range(d // LANES)], axis=0)
                to[e] = stacked.astype(BF)

    def tall_turn(t):
        tall_place(lax.rem(t + tiles - 1, tiles))
        tall_grad(t)

    def to_states(layer, a, first_slot):
        turn = 0
        for source, w, w_h in ((dgate, wg, wg_h), (dup, wu, wu_h)):
            for r in range(0, tokens, tokens // 2):
                at_rows = pl.ds(r, tokens // 2)
                part = nt(source[0, at_rows, :], w[0])
                for t in range(1, tiles):
                    part += nt(source[t, at_rows, :], w[t])
                if source is dgate:
                    a[at_rows, :] = part.astype(BF)
                else:
                    acc[at_rows, :] = part
                if turn < 3:
                    slot(first_slot + turn)
                    turn += 1
            which = 0 if source is dgate else 1
            for t in range(tiles):
                wide_weight(which, layer - 1, jnp.int32(t)).start()

        for r in range(0, tokens, 128):
            at_rows = pl.ds(r, 128)
            by_a = (a[at_rows, :].astype(F32) + acc[at_rows, :].astype(BF).astype(F32)).astype(BF).astype(F32)
            wide = h[at_rows, :].astype(F32)
            scale = lax.rsqrt(jnp.mean(wide * wide, -1, keepdims=True) + 1e-6)
            along = jnp.mean(by_a * wide, -1, keepdims=True)
            by_h = (by_a * scale - wide * (scale * scale * scale * along)).astype(BF)
            dy[at_rows, :] = (dy[at_rows, :].astype(F32) + by_h.astype(F32)).astype(BF)
        slot(first_slot + turn)

    for i in range(parts):
        load_x[i].wait()
        if i == parts - 1:
            for t in range(1, tiles):
                start(wide_weights(0, jnp.int32(t)))
            load_dy.start()
            start(first)
        for r in range(i * some, (i + 1) * some, 128):
            a0[r : r + 128, :] = normed(h[r : r + 128, :])

    def ahead(t):
        wait(wide_weights(0, t))
        next_tall(0, t, t, layers - 1)
        forward(lax.rem(t, 2), a0, t)
        start(wide_weights(layers - 1, t))

    each_tile(ahead)

    for r in range(0, tokens, 128):
        new = (h[r : r + 128, :].astype(F32) + acc[r : r + 128, :].astype(BF).astype(F32)).astype(BF)
        h[r : r + 128, :] = new
        new = normed(new)
        a1[r : r + 128, :] = new
        at[:, r : r + 128] = new.T
    load_dy.wait()
    wait(first)
    meet(n - 1)

    for step in range(layers):
        layer = layers - 1 - step
        base = step * per_layer
        a = (a0, a1)[layer]

        def tile(t, layer=layer, base=base, a=a, step=step):
            turn = (step + 1) * tiles + t
            wait(wide_weights(layer, t))
            next_tall(layer, t, turn, layer - 1 if layer > 0 else None)
            chunk = base + 2 * t
            elementwise(lax.rem(turn, 2), a, t)
            wide_grad(dgate, chunk, t)
            if step == 0:
                filling(chunk)
                wide_grad(dup, chunk + 1, t)

                @pl.when(t + 1 < tiles)
                def _():
                    filling(chunk + 1)

            else:
                slot(chunk)
                tall_place(lax.rem(t + tiles - 1, tiles))
                wide_grad(dup, chunk + 1, t)
                tall_grad(t)
                slot(chunk + 1)

        each_tile(tile)
        if step > 0:
            tall_place(jnp.int32(tiles - 1))
        if step == 0:

            def down(t, base=base):
                tall_turn(t)

                @pl.when(t == 1)
                def _():
                    slot(base + 2 * tiles - 1)

            each_tile(down)
            tall_place(jnp.int32(tiles - 1))
            slot(base + 2 * tiles)
            to_states(layer, a, base + 2 * tiles + 1)
            at[...] = a0[...].T

    def rest(turn_of):
        def body(i, _):
            turn_of(i)
            return 0

        return body

    lax.fori_loop((layers - 1) * per_layer + 2 * tiles, chunks, rest(slot), 0)
    lax.fori_loop(chunks, chunks + full, rest(emptying), 0)

    everyone[me] = jnp.sum(squares[...], axis=0, keepdims=True)

    def share(i, source):
        return pltpu.make_async_remote_copy(
            src_ref=everyone.at[source],
            dst_ref=everyone.at[source],
            send_sem=s_send.at[i],
            recv_sem=s_recv.at[i],
            device_id={"dp": others[i]},
            device_id_type=MESH,
        )

    for i in range(n - 1):
        share(i, me).start()
    for i in range(n - 1):
        share(i, lax.rem(me + n - steps_away[i], n)).wait_recv()
    square[...] = jnp.sum(everyone[...], axis=0)
    for i in range(n - 1):
        share(i, me).wait_send()


def backward(n, x, dy, wg, wu, wd, m, v):
    layers, d, ff = wg.shape
    tokens = dy.shape[0]
    tiles, rows, chips, half = ff // TILE, d // n, n // 2, n // 4
    chunks = 3 * layers * tiles
    unit = (2, 2, rows, LANES)
    hbm, vmem = pl.BlockSpec(memory_space=pl.ANY), pl.BlockSpec(memory_space=pltpu.VMEM)
    return pl.pallas_call(
        functools.partial(backward_kernel, n, layers, tiles, rows),
        in_specs=[hbm] * 7,
        out_specs=[vmem] * 5,
        out_shape=[pltpu.VMEM((chunks,) + unit, BF), pltpu.VMEM((1, LANES), F32)]
        + [pltpu.VMEM((rows, ff), dt) for dt in (BF, F32, F32)],
        scratch_shapes=[
            pltpu.VMEM((tokens, d), BF),
            pltpu.VMEM((tokens, d), BF),
            pltpu.VMEM((tokens, d), BF),
            pltpu.VMEM((d, tokens), BF),
            pltpu.VMEM((tokens, d), BF),
            pltpu.VMEM((tiles, d, TILE), BF),
            pltpu.VMEM((tiles, d, TILE), BF),
            pltpu.VMEM((2, TILE, d), BF),
            pltpu.VMEM((tiles, tokens, TILE), BF),
            pltpu.VMEM((tiles, tokens, TILE), BF),
            pltpu.VMEM((tiles, tokens, TILE), BF),
            pltpu.VMEM((tokens, d), F32),
            pltpu.VMEM((RING_GRAD + tiles, 2, chips) + unit, BF),
            pltpu.VMEM((RING_PARTNER, chips) + unit, BF),
            pltpu.VMEM((RING_SUM, chips) + unit, BF),
            pltpu.VMEM((2, LAG, 2 * half - 1) + unit[1:], BF),
            pltpu.VMEM((2, 2 * LAG, 2 * half - 1) + unit[1:], BF),
            pltpu.VMEM((rows, LANES), F32),
            pltpu.VMEM((n, 1, LANES), F32),
            pltpu.SemaphoreType.DMA((RING_PARTNER,)),
            pltpu.SemaphoreType.DMA((RING_PARTNER,)),
            pltpu.SemaphoreType.DMA((2, LAG)),
            pltpu.SemaphoreType.DMA((2, 2 * LAG)),
            pltpu.SemaphoreType.DMA((n - 1,)),
            pltpu.SemaphoreType.DMA((n - 1,)),
            pltpu.SemaphoreType.DMA((4,)),
            pltpu.SemaphoreType.DMA((5,)),
            pltpu.SemaphoreType.DMA((2, tiles)),
            pltpu.SemaphoreType.DMA((2,)),
        ],
        compiler_params=pltpu.CompilerParams(collective_id=0, has_side_effects=True, vmem_limit_bytes=VMEM_LIMIT),
        name="backward",
    )(x, dy, wg, wu, wd, m, v)


def update_kernel(n, layers, tiles, count, *refs):
    grads, square = refs[:2]
    first = refs[2:5]
    w_h, m_h, v_h = refs[5:8], refs[8:11], refs[11:14]
    w_out, m_in, v_in = refs[14:17], refs[17:20], refs[20:23]
    w_in = refs[23:26]
    load_sem, r_send, r_recv, d_send, d_recv = refs[26:]
    chips, half = n // 2, n // 4
    me, z, c, partner, plus, minus = places(n)
    per_layer = grads.shape[0] // layers
    pieces = [(layer, i) for layer in range(layers) for i in range(3)]

    def own(ref, layer, i):
        rows = m_in[i].shape[1]
        return ref.at[layer, pl.ds(pl.multiple_of(me * rows, 8), rows), :]

    greet([partner, plus, minus])
    loads = [[]]
    for p, (layer, i) in enumerate(pieces):
        if p == 0:
            continue
        loads.append(
            [
                pltpu.make_async_copy(own(w_h[i], layer, i), w_in[i].at[layer], load_sem.at[p, 0]),
                pltpu.make_async_copy(m_h[i].at[layer], m_in[i].at[layer], load_sem.at[p, 1]),
                pltpu.make_async_copy(v_h[i].at[layer], v_in[i].at[layer], load_sem.at[p, 2]),
            ]
        )
        for one in loads[-1]:
            one.start()
    factor = jnp.minimum(1.0, 0.5 * lax.rsqrt(jnp.sum(square[...]) / count + 1e-30))

    def step(w, m, v, g):
        g = g.astype(F32) * factor
        m = 0.9 * m + 0.1 * g
        v = 0.95 * v + 0.05 * g * g
        w = w.astype(F32)
        return (w - 0.02 * (m * lax.rsqrt(v + 1e-8) + 0.1 * w)).astype(BF), m, v

    def block(ref, p, chip, core, part=None):
        layer, i = pieces[p]
        rows, cols = m_in[i].shape[1:]
        start = (chip * 2 + core) * rows
        if part is None:
            return ref.at[layer, pl.ds(pl.multiple_of(start, 8), rows), :]
        if i == 2:
            return ref.at[layer, pl.ds(pl.multiple_of(start + part * (rows // 2), 8), rows // 2), :]
        return ref.at[layer, pl.ds(pl.multiple_of(start, 8), rows), pl.ds(part * (cols // 2), cols // 2)]

    def part_of(ref, p, part):
        layer, i = pieces[p]
        rows, cols = m_in[i].shape[1:]
        if i == 2:
            return ref.at[layer, pl.ds(part * (rows // 2), rows // 2), :]
        return ref.at[layer, :, pl.ds(part * (cols // 2), cols // 2)]

    def hop(way, s, p):
        i = pieces[p][1]
        chip = lax.rem(z + (chips - s if way == 0 else s), chips)
        part = way if s == half - 1 else None
        dst = block(w_out[i], p, chip, c, part)
        if s == 0:
            src = w_in[i].at[pieces[p][0]] if part is None else part_of(w_in[i], p, part)
        else:
            src = dst
        return pltpu.make_async_remote_copy(
            src_ref=src,
            dst_ref=dst,
            send_sem=r_send.at[way, s, p],
            recv_sem=r_recv.at[way, s, p],
            device_id={"dp": plus if way == 0 else minus},
            device_id_type=MESH,
        )

    def across(j, p):
        i = pieces[p][1]
        if j == 0:
            src, dst = w_in[i].at[pieces[p][0]], block(w_out[i], p, z, c)
        else:
            s, way = (j - 1) // 2, (j - 1) % 2
            chip = lax.rem(z + (chips - 1 - s if way == 0 else 1 + s), chips)
            dst = block(w_out[i], p, chip, c, way if s == half - 1 else None)
            src = dst
        return pltpu.make_async_remote_copy(
            src_ref=src,
            dst_ref=dst,
            send_sem=d_send.at[j, p],
            recv_sem=d_recv.at[j, p],
            device_id={"dp": partner},
            device_id_type=MESH,
        )

    for p, (layer, i) in enumerate(pieces):
        for one in loads[p]:
            one.wait()
        base = (layers - 1 - layer) * per_layer
        rows, cols = m_in[i].shape[1:]
        w1, m1, v1 = w_in[i], m_in[i], v_in[i]
        if i < 2:

            def column(q, _, base=base, layer=layer, i=i, w1=w1, m1=m1, v1=v1, p=p):
                t, r = q // QUARTERS, lax.rem(q, QUARTERS)
                at_cols = pl.ds(pl.multiple_of(q * LANES, LANES), LANES)
                g = grads[base + 2 * t + i, r // 2, lax.rem(r, 2)]
                old = [one[:, at_cols] for one in first] if p == 0 else [one[layer, :, at_cols] for one in (w1, m1, v1)]
                w, m, v = step(*old, g)
                w1[layer, :, at_cols] = w
                m1[layer, :, at_cols] = m
                v1[layer, :, at_cols] = v
                return 0

            lax.fori_loop(0, cols // LANES, column, 0, unroll=5)
        else:

            def row(j, _, base=base, layer=layer, w1=w1, m1=m1, v1=v1):
                at_rows = pl.ds(pl.multiple_of(j * 32, 32), 32)
                g = grads[base + 2 * tiles + j].astype(F32)
                eights = [g[r // 2, r % 2] for r in range(4)]
                g = jnp.concatenate(
                    [jnp.concatenate([e[8 * q : 8 * q + 8, :] for q in range(cols // LANES)], axis=1) for e in eights], axis=0
                )
                w, m, v = step(w1[layer, at_rows, :], m1[layer, at_rows, :], v1[layer, at_rows, :], g)
                w1[layer, at_rows, :] = w
                m1[layer, at_rows, :] = m
                v1[layer, at_rows, :] = v
                return 0

            lax.fori_loop(0, rows // 32, row, 0, unroll=5)
        if p == 0:
            meet(3)
        for way in (0, 1):
            hop(way, 0, p).start()
        across(0, p).start()
        start = pl.ds(pl.multiple_of(me * rows, 8), rows)
        w_out[i][layer, start, :] = w1[layer]
    def settle(s, p):
        for way in (0, 1):
            hop(way, s, p).wait_send()
            across(1 + 2 * s + way, p).wait()

    for s in range(1, half + 1):
        for p in range(len(pieces)):
            if s == half:
                across(0, p).wait()
                for early in range(half - 1):
                    settle(early, p)
            for way in (0, 1):
                hop(way, s - 1, p).wait_recv()
                if s < half:
                    hop(way, s, p).start()
                across(1 + 2 * (s - 1) + way, p).start()
    for p in range(len(pieces)):
        settle(half - 1, p)


def update(n, grads, square, first, ws, ms, vs):
    layers, d, ff = ws[0].shape
    half = n // 4
    pieces = 3 * layers
    tiles = ff // TILE
    hbm, vmem = pl.BlockSpec(memory_space=pl.ANY), pl.BlockSpec(memory_space=pltpu.VMEM)
    count = sum(w.size for w in ws)
    like = lambda t, dt=None: jax.ShapeDtypeStruct(t.shape, dt or t.dtype)
    return pl.pallas_call(
        functools.partial(update_kernel, n, layers, tiles, count),
        in_specs=[vmem] * 5 + [hbm] * 9,
        out_specs=[vmem] * 9,
        out_shape=[pltpu.VMEM(t.shape, t.dtype) for t in (*ws, *ms, *vs)],
        scratch_shapes=[pltpu.VMEM(m.shape, BF) for m in ms]
        + [
            pltpu.SemaphoreType.DMA((pieces, 3)),
            pltpu.SemaphoreType.DMA((2, half, pieces)),
            pltpu.SemaphoreType.DMA((2, half, pieces)),
            pltpu.SemaphoreType.DMA((1 + 2 * half, pieces)),
            pltpu.SemaphoreType.DMA((1 + 2 * half, pieces)),
        ],
        compiler_params=pltpu.CompilerParams(collective_id=1, has_side_effects=True, vmem_limit_bytes=4_000_000),
        name="update",
    )(
        *(pltpu.with_memory_space_constraint(t, pltpu.VMEM) for t in (grads, square, *first)),
        *(pltpu.with_memory_space_constraint(t, pltpu.HBM) for t in (*ws, *ms, *vs)),
    )


def place_kernel(*refs):
    k = len(refs) // 2
    sems = refs[-1]
    layers = refs[0].shape[0]
    copies = [pltpu.make_async_copy(refs[i].at[j], refs[k + i].at[j], sems.at[i, j]) for j in range(layers) for i in range(k)]
    for one in copies:
        one.start()
    for one in copies:
        one.wait()


def place(arrays):
    hbm, vmem = pl.BlockSpec(memory_space=pl.ANY), pl.BlockSpec(memory_space=pltpu.VMEM)
    return pl.pallas_call(
        place_kernel,
        in_specs=[vmem] * len(arrays),
        out_specs=[hbm] * len(arrays),
        out_shape=[pltpu.HBM(t.shape, t.dtype) for t in arrays],
        scratch_shapes=[pltpu.SemaphoreType.DMA((len(arrays), arrays[0].shape[0]))],
        compiler_params=pltpu.CompilerParams(vmem_limit_bytes=1_000_000),
        name="place",
    )(*(pltpu.with_memory_space_constraint(t, pltpu.VMEM) for t in arrays))


def solution(mesh):
    n = mesh.shape["dp"]

    def of_a_device(x, dy, *arrays):
        ws, ms, vs = (arrays[i : i + 3] for i in (0, 3, 6))
        grads, square, *first = backward(n, x[0], dy[0], *ws, ms[0], vs[0])
        return tuple(place(update(n, grads, square, first, ws, ms, vs)))

    seq, whole, rows = P(("rep", "dp")), P(), P(None, "dp")
    return jax.shard_map(
        of_a_device,
        mesh=mesh,
        in_specs=(seq, seq) + (whole,) * 3 + (rows,) * 6,
        out_specs=(P("rep"),) * 3 + (P("rep", "dp"),) * 6,
        check_vma=False,
    )
```
